256 devices in a mesh: seq: 32 (over y, x, core), head: 8 (over z).
Axes of the slice: x: 4, y: 4, z: 8, core: 2. Of those that a mesh axis runs over, the one named last changes fastest.
Arguments:
- queries: bfloat16 [4096, 64, 128], P('seq', 'head'), may hold values from -150 to 150
- key_store: bfloat16 [4096, 8, 128], P(('seq', 'head')), may hold values from -5.2 to 5.2
- value_store: bfloat16 [4096, 8, 128], P(('seq', 'head')), may hold values from -6 to 6
- upstream: bfloat16 [4096, 64, 128], P('seq', 'head'), may hold values from -5 to 5
- fork_pages: int32 [32, 8], P('seq'), may hold values from 0 to 31, as said below
- fork_visible: int32 [32, 8], P('seq'), may hold values from 1 to 128
Outputs:
- attended: bfloat16 [4096, 64, 128], P('seq', 'head')
- query_grad: bfloat16 [4096, 64, 128], P('seq', 'head')
- key_grad: bfloat16 [4096, 8, 128], P(('seq', 'head'))
- value_grad: bfloat16 [4096, 8, 128], P(('seq', 'head'))
The draws below stay inside these ranges and needn't reach their ends.
Inputs may be any that keep to these rules, and one draw needn't show every extreme that they name: `fork_pages`: page p is held by seq index p. The 8 entries of the blocks of one seq index never name its own pages; at most 2 of them name pages held by any one other seq index, and exactly 2 name pages held by some one other seq index.
All inputs are finite; a program needn't handle non-finite values.
Results may differ from the reference program's by a relative error of at most 0.019.
Values may be sent and summed in bfloat16 or wider, within the bound.
A program may use at most 64 MiB of HBM per device.

```python
import math
import jax
import jax.numpy as jnp
from jax import lax

QH = 64
KVH = 8
HD = 128
BLK = 128
FORKS = 8
BLK_DEV = 1
NBLK = 32
TOKENS = 4096
MOST = 2
N_SEQ = 32


def base_keys(key):
    raw = jax.random.normal(jax.random.fold_in(key, 11), (TOKENS, KVH, HD), jnp.float32)
    return jnp.clip(raw, -5.0, 5.0)


def draw_key_store(key, part):
    raw = base_keys(key)
    return raw.astype(jnp.bfloat16)


def draw_queries(key, part):
    raw = jnp.clip(jax.random.normal(jax.random.fold_in(key, 12), (TOKENS, QH, HD), jnp.float32), -5.0, 5.0)
    return raw.astype(jnp.bfloat16)


def draw_upstream(key, part):
    raw = jnp.clip(jax.random.normal(jax.random.fold_in(key, 14), (TOKENS, QH, HD), jnp.float32), -5.0, 5.0)
    return raw.astype(jnp.bfloat16)


def draw_fork_pages(key, part):
    entries = BLK_DEV * FORKS
    split = jax.random.split(jax.random.fold_in(key, 13), 4)
    busiest = jax.random.randint(split[0], (N_SEQ, 1), 0, N_SEQ - 1)
    slot_order = jax.vmap(lambda sub: jax.random.permutation(sub, (N_SEQ - 2) * MOST))(jax.random.split(split[1], N_SEQ))
    others = (busiest + 1 + slot_order[:, :entries - MOST] // MOST) % (N_SEQ - 1)
    relative = jnp.concatenate([jnp.broadcast_to(busiest, (N_SEQ, MOST)), others], axis=1)
    shuffle = jax.vmap(lambda sub: jax.random.permutation(sub, entries))(jax.random.split(split[2], N_SEQ))
    relative = jnp.take_along_axis(relative, shuffle, axis=1)
    holders = (jnp.arange(N_SEQ)[:, None] + 1 + relative) % N_SEQ
    within = jax.random.randint(split[3], (N_SEQ, entries), 0, BLK_DEV)
    return (holders * BLK_DEV + within).reshape(NBLK, FORKS).astype(jnp.int32)


def with_ends(values, own_key, least, high):
    longest = values.shape.index(max(values.shape))
    spots = []
    for shift in (0, 1):
        where = [jax.random.randint(jax.random.fold_in(own_key, axis), (), 0, length) for axis, length in enumerate(values.shape)]
        where[longest] = (where[longest] + shift) % values.shape[longest]
        spots.append(tuple(where))
    return values.at[spots[0]].set(least).at[spots[1]].set(high)


def level_of(own_key, shape, cuts, low, high):
    def one(axis_at, parts):
        steps = jax.random.uniform(jax.random.fold_in(jax.random.fold_in(own_key, 6), axis_at), (parts,), jnp.float32, low / len(cuts), high / len(cuts))
        return jnp.repeat(jnp.exp(steps), shape[axis_at] // parts).reshape((-1,) + (1,) * (len(shape) - axis_at - 1))

    factor_of = one(*cuts[0])
    for cut in cuts[1:]:
        factor_of = factor_of * one(*cut)
    return factor_of


def noise(stream_key, extent, scale, bound, cuts=(), held_as=jnp.bfloat16):
    values = jax.random.normal(stream_key, extent, jnp.float32) * scale
    if len(cuts) > 0:
        values = level_of(stream_key, extent, cuts, -0.22, 0.18) * values
    return jnp.clip(values, min=-bound, max=bound).astype(held_as)


def setup_inputs(seed: int = 0) -> dict:
    splits = jax.random.split(jax.random.key(seed), 7)
    return {
        "queries": draw_queries(jax.random.fold_in(splits[6], 71), 0),
        "key_store": draw_key_store(jax.random.fold_in(splits[6], 71), 0),
        "value_store": noise(splits[2], (TOKENS, KVH, HD), 1.0, 6.0, ((0, 256),)),
        "upstream": draw_upstream(jax.random.fold_in(splits[6], 71), 0),
        "fork_pages": draw_fork_pages(jax.random.fold_in(splits[6], 71), 0),
        "fork_visible": with_ends(jax.random.randint(splits[5], (NBLK, FORKS), 1, BLK + 1), jax.random.fold_in(splits[5], 1), 1, BLK).astype(jnp.int32),
    }


HIGH = lax.Precision.HIGHEST

def attend_block(query_blk, grad_blk, key_cat, value_cat, fork_limit):
    row_total, head_total, head_dim = query_blk.shape
    kv_total = key_cat.shape[1]
    groups = head_total // kv_total
    factor = 1.0 / math.sqrt(head_dim)
    query_grid = query_blk.reshape(row_total, kv_total, groups, head_dim).astype(jnp.float32)
    grad_grid = grad_blk.reshape(row_total, kv_total, groups, head_dim).astype(jnp.float32)
    key_wide = key_cat.astype(jnp.float32)
    value_wide = value_cat.astype(jnp.float32)
    scores = jnp.einsum('qkgd,skd->kgqs', query_grid, key_wide, precision=HIGH) * factor
    positions = jnp.arange(row_total, dtype=jnp.int32)
    causal = positions[None, :] <= positions[:, None]
    fork_part = (positions[None, :] < fork_limit[:, None]).reshape(-1)
    allowed = jnp.concatenate([causal, jnp.broadcast_to(fork_part[None, :], (row_total, fork_part.shape[0]))], axis=1)
    scores = jnp.where(allowed, scores, -1e+30)
    row_max = lax.optimization_barrier(jnp.max(scores, axis=-1, keepdims=True))
    exp_scores = jnp.where(allowed, jnp.exp(scores - row_max), 0.0)
    weights = exp_scores / lax.optimization_barrier(jnp.sum(exp_scores, axis=-1, keepdims=True))
    weights_b = weights.astype(jnp.bfloat16).astype(jnp.float32)
    attended = jnp.einsum('kgqs,skd->qkgd', weights_b, value_wide, precision=HIGH).astype(jnp.bfloat16)
    row_delta = lax.optimization_barrier(jnp.sum(grad_grid * attended.astype(jnp.float32), axis=-1))
    weight_grad = jnp.einsum('qkgd,skd->kgqs', grad_grid, value_wide, precision=HIGH)
    score_grad = (weights * (weight_grad - jnp.transpose(row_delta, (1, 2, 0))[..., None])).astype(jnp.bfloat16).astype(jnp.float32)
    query_grad = (jnp.einsum('kgqs,skd->qkgd', score_grad, key_wide, precision=HIGH) * factor).astype(jnp.bfloat16)
    key_grad = jnp.einsum('kgqs,qkgd->skd', score_grad, query_grid, precision=HIGH) * factor
    value_grad = jnp.einsum('kgqs,qkgd->skd', weights_b, grad_grid, precision=HIGH)
    return (attended.reshape(row_total, head_total, head_dim), query_grad.reshape(row_total, head_total, head_dim), key_grad, value_grad)

def reference(queries, key_store, value_store, upstream, fork_pages, fork_visible):
    key_pages = key_store.reshape(NBLK, BLK, KVH, HD)
    value_pages = value_store.reshape(NBLK, BLK, KVH, HD)
    query_blocks = queries.reshape(NBLK, BLK, QH, HD)
    grad_blocks = upstream.reshape(NBLK, BLK, QH, HD)

    def advance(sums, block_id):
        key_total, value_total = sums
        ancestors = fork_pages[block_id].astype(jnp.int32)
        targets = jnp.concatenate([block_id[None], ancestors]).astype(jnp.int32)
        key_cat = key_pages[targets].reshape(-1, KVH, HD)
        value_cat = value_pages[targets].reshape(-1, KVH, HD)
        attended, query_grad, key_grad, value_grad = attend_block(query_blocks[block_id], grad_blocks[block_id], key_cat, value_cat, fork_visible[block_id])
        key_total = key_total.at[targets].add(key_grad.reshape(FORKS + 1, BLK, KVH, HD))
        value_total = value_total.at[targets].add(value_grad.reshape(FORKS + 1, BLK, KVH, HD))
        return ((key_total, value_total), (attended, query_grad))
    empty_sum = jnp.zeros((NBLK, BLK, KVH, HD), jnp.float32)
    (key_total, value_total), (attended, query_grad) = lax.scan(advance, (empty_sum, empty_sum), jnp.arange(NBLK, dtype=jnp.int32))
    return (attended.reshape(TOKENS, QH, HD), query_grad.reshape(TOKENS, QH, HD), key_total.reshape(TOKENS, KVH, HD).astype(jnp.bfloat16), value_total.reshape(TOKENS, KVH, HD).astype(jnp.bfloat16))
```

```python
import functools
import math

import jax
import jax.numpy as jnp
from jax import lax
from jax.experimental import pallas as pl
from jax.experimental.pallas import tpu as pltpu
from jax.sharding import PartitionSpec as P

HD = 128
BLK = 128
FORKS = 8
ENT = FORKS + 1
CW = 256
F32 = jnp.float32
BF16 = jnp.bfloat16
MESH = pl.DeviceIdType.MESH
NT = (((1,), (1,)), ((), ()))
FACTOR = 1.0 / math.sqrt(HD)
LOG2E = 1.4426950408889634
NEG = -1e30


def dot(a, b):
    return jnp.dot(a, b, preferred_element_type=F32)


def dot_nt(a, b):
    return lax.dot_general(a, b, NT, preferred_element_type=F32)


def remote(src, dst, send_sem, recv_sem, seq, head):
    return pltpu.make_async_remote_copy(
        src_ref=src, dst_ref=dst, send_sem=send_sem, recv_sem=recv_sem,
        device_id=(seq, head), device_id_type=MESH,
    )


def kernel(
    nx, ny, nz, groups,
    fork_ref, vis_ref, k_ref, v_ref, q_hbm, g_hbm,
    att_hbm, qg_hbm, kg_ref, vg_ref,
    q_buf, g_buf, gt_buf, att_buf, qg_buf, delta_buf,
    zsrc, kpages, vpages, ksel, vsel, kt_sel, vt_sel, s_buf,
    acc, slot_of, dsend, prec, rsend, rrec, fin, zrec,
    io_sem, z_send, z_recv, ag_send, ag_recv, fw_send, fw_recv,
    dd_send, dd_recv, rs_send, rs_recv, zb_send, zb_recv,
):
    nc = nx * ny
    rows = BLK * groups
    chunks = rows // CW
    sub = BLK // nz
    seq = lax.axis_index("seq")
    z = lax.axis_index("head")
    core = lax.rem(seq, 2)
    chip = seq // 2
    x = lax.rem(chip, nx)
    y = chip // nx
    partner = chip * 2 + (1 - core)

    def ring(d, n):
        return min(d, n - d)

    offsets = [(dx, dy) for dy in range(ny) for dx in range(nx)]
    far = sorted(range(1, nc), key=lambda o: -(ring(offsets[o][0], nx) + ring(offsets[o][1], ny)))
    near = far[::-1]

    def chip_at(o, sign):
        dx, dy = offsets[o]
        tx = lax.rem(x + (dx if sign > 0 else nx - dx), nx)
        ty = lax.rem(y + (dy if sign > 0 else ny - dy), ny)
        return ty * nx + tx

    load_q = pltpu.make_async_copy(q_hbm, q_buf, io_sem.at[0])
    load_g = pltpu.make_async_copy(g_hbm, g_buf, io_sem.at[1])
    load_g.start()
    load_q.start()

    barrier = pltpu.get_barrier_semaphore()
    for o in range(1, nz):
        pl.semaphore_signal(barrier, inc=1, device_id=(seq, lax.rem(z + o, nz)), device_id_type=MESH)
    for o in far:
        pl.semaphore_signal(barrier, inc=1, device_id=(chip_at(o, 1) * 2 + core, z), device_id_type=MESH)
    pl.semaphore_signal(barrier, inc=1, device_id=(partner, z), device_id_type=MESH)

    r0 = lax.broadcasted_iota(jnp.int32, (BLK, BLK), 0)
    r1 = lax.broadcasted_iota(jnp.int32, (BLK, BLK), 1)
    to_heads = (r1 == lax.rem(r0, sub) * nz + r0 // sub).astype(BF16)
    to_tokens = (r1 == lax.rem(r0, nz) * sub + r0 // nz).astype(BF16)
    pages = (kpages, vpages)
    for t, ref in enumerate((k_ref, v_ref)):
        zsrc[t] = dot(to_heads, ref[...]).astype(BF16).reshape(nz, sub, HD)
        pages[t][seq, z] = zsrc[t, z]

    pl.semaphore_wait(barrier, nz - 1 + nc - 1 + 1)

    def z_copy(t, o):
        head = lax.rem(z + o, nz)
        return remote(zsrc.at[t, head], pages[t].at[seq, z], z_send.at[t, o], z_recv.at[t, o], seq, head)

    z_order = sorted(range(1, nz), key=lambda o: -ring(o, nz))
    for t in range(2):
        for o in z_order:
            z_copy(t, o).start()

    def entry_slots(p, _):
        first = jnp.int32(ENT)
        second = jnp.int32(ENT)
        for e in range(FORKS):
            hit = fork_ref[0, e] == p
            second = jnp.where(hit & (first < ENT), e + 1, second)
            first = jnp.where(hit & (first == ENT), e + 1, first)
        slot_of[0, p] = first
        slot_of[1, p] = second
        return 0

    lax.fori_loop(0, 2 * nc, entry_slots, 0)
    acc[0, ENT] = jnp.zeros((BLK, HD), F32)
    acc[1, ENT] = jnp.zeros((BLK, HD), F32)

    load_g.wait()
    for c in range(chunks):
        gt_buf[c] = g_buf[c * CW:(c + 1) * CW, :].T

    def z_wait(t):
        for o in z_order[::-1]:
            head = lax.rem(z + nz - o, nz)
            here = pages[t].at[seq, head]
            remote(here, here, z_send.at[t, o], z_recv.at[t, o], seq, head).wait_recv()

    def page_send(t, o):
        ref = pages[t].at[seq]
        return remote(ref, ref, ag_send.at[t, o], ag_recv.at[t, o], chip_at(o, 1) * 2 + core, z)

    def page_forward(t, o):
        ref = pages[t].at[chip_at(o, -1) * 2 + core] if o else pages[t].at[seq]
        return remote(ref, ref, fw_send.at[t, o], fw_recv.at[t, o], partner, z)

    def page_arrival(t, o):
        src = chip_at(o, -1) * 2 + core
        ref = pages[t].at[src]
        return remote(ref, ref, ag_send.at[t, o], ag_recv.at[t, o], src, z)

    def forward_arrival(t, o):
        ref = pages[t].at[chip_at(o, -1) * 2 + (1 - core)] if o else pages[t].at[partner]
        return remote(ref, ref, fw_send.at[t, o], fw_recv.at[t, o], partner, z)

    for t in range(2):
        z_wait(t)
        for o in far:
            page_send(t, o).start()
        page_forward(t, 0).start()

    def collect(t):
        for o in near:
            page_arrival(t, o).wait_recv()
            page_forward(t, o).start()
        for o in [0] + near:
            forward_arrival(t, o).wait_recv()

    def select_pages(t, sel, sel_t):
        for e in range(ENT):
            page = pages[t][seq] if e == 0 else pages[t][fork_ref[0, e - 1]]
            page = page.reshape(BLK, HD)
            sel[e] = page
            sel_t[:, e * BLK:(e + 1) * BLK] = page.T

    collect(0)
    select_pages(0, ksel, kt_sel)
    load_q.wait()

    key_row = lax.broadcasted_iota(jnp.int32, (BLK, CW), 0)
    col = lax.broadcasted_iota(jnp.int32, (BLK, CW), 1)

    def halves(a):
        return a.reshape(BLK // 8, 8, CW)

    def scores(c, _):
        q_c = q_buf[pl.ds(pl.multiple_of(c * CW, CW), CW), :]
        top = jnp.full((8, CW), NEG, F32)
        for e in range(ENT):
            raw = dot_nt(ksel[e], q_c) * (FACTOR * LOG2E)
            if e == 0:
                seen = key_row <= (col + c * CW) // groups
            else:
                seen = key_row < vis_ref[0, e - 1]
            raw = jnp.where(seen, raw, NEG)
            s_buf[c, e] = raw
            top = jnp.maximum(top, jnp.max(halves(raw), axis=0))
        top = jnp.max(top, axis=0, keepdims=True)
        total = jnp.zeros((8, CW), F32)
        for e in range(ENT):
            expo = jnp.exp2(s_buf[c, e] - top)
            s_buf[c, e] = expo
            total = total + jnp.sum(halves(expo), axis=0)
        delta_buf[c] = jnp.broadcast_to(1.0 / jnp.sum(total, axis=0, keepdims=True), (8, CW))
        return 0

    lax.fori_loop(0, chunks, scores, 0)

    collect(1)
    select_pages(1, vsel, vt_sel)

    for e in range(ENT):
        acc[0, e] = jnp.zeros((BLK, HD), F32)
        acc[1, e] = jnp.zeros((BLK, HD), F32)

    def values(c, _):
        rows_c = pl.ds(pl.multiple_of(c * CW, CW), CW)
        g_c = g_buf[rows_c, :]
        inverse = delta_buf[c][:1]
        out_t = jnp.zeros((HD, CW), F32)
        for e in range(ENT):
            w = s_buf[c, e] * inverse
            s_buf[c, e] = w
            w_b = w.astype(BF16)
            out_t = out_t + dot(vt_sel[:, e * BLK:(e + 1) * BLK], w_b)
            acc[1, e] += dot(w_b, g_c)
        out_b = out_t.astype(BF16)
        att_buf[rows_c, :] = out_b.T
        delta = jnp.sum(out_b.astype(F32) * gt_buf[c].astype(F32), axis=0, keepdims=True)
        delta_buf[c] = jnp.broadcast_to(delta, (8, CW))
        return 0

    lax.fori_loop(0, chunks, values, 0)
    store_att = pltpu.make_async_copy(att_buf, att_hbm, io_sem.at[2])
    store_att.start()

    def slot_sum(t, page):
        return acc[t, slot_of[0, page]] + acc[t, slot_of[1, page]]

    def partner_send(t, o):
        return remote(dsend.at[t, o], prec.at[t, o], dd_send.at[t, o], dd_recv.at[t, o], partner, z)

    def reduce_send(t, o):
        return remote(rsend.at[t, o], rrec.at[t, o], rs_send.at[t, o], rs_recv.at[t, o], chip_at(o, 1) * 2 + core, z)

    def to_partner(t):
        for o in far + [0]:
            dsend[t, o] = slot_sum(t, chip_at(o, 1) * 2 + (1 - core)).astype(BF16)
            partner_send(t, o).start()

    def to_chips(t):
        for o in far:
            partner_send(t, o).wait_recv()
            mine = slot_sum(t, chip_at(o, 1) * 2 + core) + prec[t, o].astype(F32)
            rsend[t, o] = mine.astype(BF16)
            reduce_send(t, o).start()
        partner_send(t, 0).wait_recv()

    to_partner(1)
    to_chips(1)

    def grads(c, _):
        rows_c = pl.ds(pl.multiple_of(c * CW, CW), CW)
        g_c = g_buf[rows_c, :]
        q_c = q_buf[rows_c, :]
        delta = delta_buf[c][:1]
        dq_t = jnp.zeros((HD, CW), F32)
        for e in range(ENT):
            ds = (s_buf[c, e] * (dot_nt(vsel[e], g_c) - delta)).astype(BF16)
            dq_t = dq_t + dot(kt_sel[:, e * BLK:(e + 1) * BLK], ds)
            acc[0, e] += dot(ds, q_c)
        qg_buf[rows_c, :] = (dq_t * FACTOR).T.astype(BF16)
        return 0

    lax.fori_loop(0, chunks, grads, 0)
    store_qg = pltpu.make_async_copy(qg_buf, qg_hbm, io_sem.at[3])
    store_qg.start()
    to_partner(0)
    to_chips(0)

    def zb_copy(t, o):
        head = lax.rem(z + o, nz)
        return remote(fin.at[t, head], zrec.at[t, z], zb_send.at[t, o], zb_recv.at[t, o], seq, head)

    def finish(t):
        total = acc[t, 0] + slot_sum(t, seq) + prec[t, 0].astype(F32)
        for o in near:
            reduce_send(t, o).wait_recv()
            total = total + rrec[t, o].astype(F32)
        if t == 0:
            total = total * FACTOR
        fin[t] = total.astype(BF16).reshape(nz, sub, HD)
        zrec[t, z] = fin[t, z]
        for o in z_order:
            zb_copy(t, o).start()

    def result(t, out_ref):
        for o in z_order[::-1]:
            head = lax.rem(z + nz - o, nz)
            here = zrec.at[t, head]
            remote(here, here, zb_send.at[t, o], zb_recv.at[t, o], seq, head).wait_recv()
        out_ref[...] = dot(to_tokens, zrec[t].reshape(BLK, HD)).astype(BF16)

    finish(1)
    finish(0)
    result(1, vg_ref)
    result(0, kg_ref)

    store_att.wait()
    store_qg.wait()
    for t in range(2):
        for o in range(1, nz):
            z_copy(t, o).wait_send()
            zb_copy(t, o).wait_send()
        for o in range(1, nc):
            page_send(t, o).wait_send()
            reduce_send(t, o).wait_send()
        for o in range(nc):
            page_forward(t, o).wait_send()
            partner_send(t, o).wait_send()


def per_device(nx, ny, nz, queries, key_store, value_store, upstream, fork_pages, fork_visible):
    groups = queries.shape[1]
    rows = BLK * groups
    chunks = rows // CW
    nc = nx * ny
    sub = BLK // nz
    dma = pltpu.SemaphoreType.DMA
    smem = pl.BlockSpec(memory_space=pltpu.SMEM)
    vmem = pl.BlockSpec(memory_space=pltpu.VMEM)
    hbm = pl.BlockSpec(memory_space=pl.ANY)
    big = jax.ShapeDtypeStruct((rows, HD), BF16)
    small = jax.ShapeDtypeStruct((BLK, HD), BF16)
    att, qg, kg, vg = pl.pallas_call(
        functools.partial(kernel, nx, ny, nz, groups),
        out_shape=(big, big, small, small),
        in_specs=[smem, smem, vmem, vmem, hbm, hbm],
        out_specs=(hbm, hbm, vmem, vmem),
        scratch_shapes=[
            pltpu.VMEM((rows, HD), BF16),
            pltpu.VMEM((rows, HD), BF16),
            pltpu.VMEM((chunks, HD, CW), BF16),
            pltpu.VMEM((rows, HD), BF16),
            pltpu.VMEM((rows, HD), BF16),
            pltpu.VMEM((chunks, 8, CW), F32),
            pltpu.VMEM((2, nz, sub, HD), BF16),
            pltpu.VMEM((2 * nc, nz, sub, HD), BF16),
            pltpu.VMEM((2 * nc, nz, sub, HD), BF16),
            pltpu.VMEM((ENT, BLK, HD), BF16),
            pltpu.VMEM((ENT, BLK, HD), BF16),
            pltpu.VMEM((HD, ENT * BLK), BF16),
            pltpu.VMEM((HD, ENT * BLK), BF16),
            pltpu.VMEM((chunks, ENT, BLK, CW), F32),
            pltpu.VMEM((2, ENT + 1, BLK, HD), F32),
            pltpu.SMEM((2, 2 * nc), jnp.int32),
            pltpu.VMEM((2, nc, BLK, HD), BF16),
            pltpu.VMEM((2, nc, BLK, HD), BF16),
            pltpu.VMEM((2, nc, BLK, HD), BF16),
            pltpu.VMEM((2, nc, BLK, HD), BF16),
            pltpu.VMEM((2, nz, sub, HD), BF16),
            pltpu.VMEM((2, nz, sub, HD), BF16),
            dma((4,)),
            dma((2, nz)), dma((2, nz)),
            dma((2, nc)), dma((2, nc)),
            dma((2, nc)), dma((2, nc)),
            dma((2, nc)), dma((2, nc)),
            dma((2, nc)), dma((2, nc)),
            dma((2, nz)), dma((2, nz)),
        ],
        compiler_params=pltpu.CompilerParams(collective_id=0, has_side_effects=True),
    )(
        fork_pages, fork_visible,
        key_store.reshape(BLK, HD), value_store.reshape(BLK, HD),
        queries.reshape(rows, HD), upstream.reshape(rows, HD),
    )
    return (
        att.reshape(queries.shape), qg.reshape(queries.shape),
        kg.reshape(key_store.shape), vg.reshape(value_store.shape),
    )


def solution(mesh):
    nc = mesh.shape["seq"] // 2
    nx = 1
    while nx * nx < nc:
        nx *= 2
    placed = (
        P("seq", "head", None),
        P(("seq", "head"), None, None),
        P(("seq", "head"), None, None),
        P("seq", "head", None),
        P("seq", None),
        P("seq", None),
    )
    return jax.shard_map(
        functools.partial(per_device, nx, nc // nx, mesh.shape["head"]),
        mesh=mesh,
        in_specs=placed,
        out_specs=(
            P("seq", "head", None),
            P("seq", "head", None),
            P(("seq", "head"), None, None),
            P(("seq", "head"), None, None),
        ),
        check_vma=False,
    )
```

```python
import functools
import math

import jax
import jax.numpy as jnp
from jax import lax
from jax.experimental import pallas as pl
from jax.experimental.pallas import tpu as pltpu
from jax.sharding import PartitionSpec as P

HD = 128
BLK = 128
FORKS = 8
ENT = FORKS + 1
CW = 256
F32 = jnp.float32
BF16 = jnp.bfloat16
MESH = pl.DeviceIdType.MESH
NT = (((1,), (1,)), ((), ()))
FACTOR = 1.0 / math.sqrt(HD)
LOG2E = 1.4426950408889634
NEG = -1e30


def dot(a, b):
    return jnp.dot(a, b, preferred_element_type=F32)


def dot_nt(a, b):
    return lax.dot_general(a, b, NT, preferred_element_type=F32)


def remote(src, dst, send_sem, recv_sem, seq, head):
    return pltpu.make_async_remote_copy(
        src_ref=src, dst_ref=dst, send_sem=send_sem, recv_sem=recv_sem,
        device_id=(seq, head), device_id_type=MESH,
    )


def kernel(
    nx, ny, nz, groups,
    fork_hbm, vis_hbm, k_hbm, v_hbm, q_hbm, g_hbm,
    att_hbm, qg_hbm, kg_ref, vg_ref,
    att_ref, qg_ref, kv_in, q_buf, g_buf, gt_buf, delta_buf,
    zsrc, kpages, vpages, ksel, vsel, kt_sel, vt_sel, s_buf,
    acc, fork_ref, vis_ref, slot_of, dsend, prec, rsend, rrec, ssend, srec, fin, zrec,
    io_sem, z_send, z_recv, ag_send, ag_recv, fw_send, fw_recv,
    dd_send, dd_recv, r1_send, r1_recv, r2_send, r2_recv, zb_send, zb_recv,
):
    nc = nx * ny
    rows = BLK * groups
    chunks = rows // CW
    sub = BLK // nz
    hb = BLK // 2
    hz = nz // 2
    seq = lax.axis_index("seq")
    z = lax.axis_index("head")
    core = lax.rem(seq, 2)
    chip = seq // 2
    x = lax.rem(chip, nx)
    y = chip // nx
    partner = chip * 2 + (1 - core)

    def ring(d, n):
        return min(d, n - d)

    offsets = [(dx, dy) for dy in range(ny) for dx in range(nx)]
    far = sorted(range(1, nc), key=lambda o: -(ring(offsets[o][0], nx) + ring(offsets[o][1], ny)))
    near = far[::-1]
    rel = [(j + 1) // 2 if j % 2 else (nz - j // 2) % nz for j in range(nz)]
    slot_at = {r: j for j, r in enumerate(rel)}
    bounds = [0, 1, 3, 5, 8] if nz == 8 else [0, 1, nz]
    parts = list(zip(bounds[:-1], bounds[1:]))
    part_of = [p for p, (lo, hi) in enumerate(parts) for _ in range(lo, hi)]

    def chip_at(dx, dy):
        return lax.rem(y + dy, ny) * nx + lax.rem(x + dx, nx)

    def chip_to(o):
        return chip_at(*offsets[o])

    def chip_from(o):
        dx, dy = offsets[o]
        return chip_at((nx - dx) % nx, (ny - dy) % ny)

    loads = [
        pltpu.make_async_copy(k_hbm, kv_in.at[0], io_sem.at[0]),
        pltpu.make_async_copy(v_hbm, kv_in.at[1], io_sem.at[1]),
        pltpu.make_async_copy(g_hbm, g_buf, io_sem.at[2]),
        pltpu.make_async_copy(q_hbm, q_buf, io_sem.at[3]),
        pltpu.make_async_copy(fork_hbm, fork_ref, io_sem.at[4]),
        pltpu.make_async_copy(vis_hbm, vis_ref, io_sem.at[5]),
    ]
    barrier = pltpu.get_barrier_semaphore()
    for o in range(1, nz):
        pl.semaphore_signal(barrier, inc=1, device_id=(seq, lax.rem(z + o, nz)), device_id_type=MESH)
    for o in far:
        pl.semaphore_signal(barrier, inc=1, device_id=(chip_to(o) * 2 + core, z), device_id_type=MESH)
    pl.semaphore_signal(barrier, inc=1, device_id=(partner, z), device_id_type=MESH)
    for load in loads:
        load.start()

    r0 = lax.broadcasted_iota(jnp.int32, (BLK, BLK), 0)
    r1 = lax.broadcasted_iota(jnp.int32, (BLK, BLK), 1)

    def slot_head(j):
        return lax.rem(z + jnp.where(lax.rem(j, 2) == 1, (j + 1) // 2, nz - j // 2), nz)

    to_heads = (r1 == lax.rem(r0, sub) * nz + r0 // sub).astype(BF16)
    from_slots = (lax.rem(r0, nz) == slot_head(r1 // sub)) & (r0 // nz == lax.rem(r1, sub))
    from_slots = from_slots.astype(F32).astype(BF16)
    pages = (kpages, vpages)
    for t in range(2):
        loads[t].wait()
        zsrc[t] = dot(to_heads, kv_in[t]).astype(BF16).reshape(nz, sub, HD)
        pages[t][chip, core, 0] = zsrc[t, z]

    pl.semaphore_wait(barrier, nz - 1 + nc - 1 + 1)

    def z_copy(t, o):
        head = lax.rem(z + o, nz)
        dst = pages[t].at[chip, core, slot_at[(nz - o) % nz]]
        return remote(zsrc.at[t, head], dst, z_send.at[0], z_recv.at[t, part_of[slot_at[(nz - o) % nz]]], seq, head)

    def page_part(t, page, part):
        lo, hi = parts[part]
        return pages[t].at[page // 2, lax.rem(page, 2), pl.ds(lo, hi - lo)]

    def page_send(t, part, o):
        ref = page_part(t, seq, part)
        return remote(ref, ref, ag_send.at[t], ag_recv.at[t, part], chip_to(o) * 2 + core, z)

    def page_arrivals(t, part):
        lo, hi = parts[part]
        ref = pages[t].at[pl.ds(0, nc - 1), 0, pl.ds(lo, hi - lo)]
        return remote(ref, ref, ag_send.at[t], ag_recv.at[t, part], partner, z)

    def page_forward(t, part):
        lo, hi = parts[part]
        ref = pages[t].at[pl.ds(0, nc), core, pl.ds(lo, hi - lo)]
        return remote(ref, ref, fw_send.at[t], fw_recv.at[t, part], partner, z)

    z_order = sorted(range(1, nz), key=lambda o: -ring(o, nz))
    for o in z_order:
        for t in range(2):
            z_copy(t, o).start()

    def send_part(part):
        lo, hi = parts[part]
        for t in range(2):
            if part:
                here = pages[t].at[chip, core, pl.ds(lo, hi - lo)]
                remote(here, here, z_send.at[0], z_recv.at[t, part], seq, lax.rem(z + 1, nz)).wait_recv()
            for o in far:
                page_send(t, part, o).start()

    send_part(0)

    def entry_slots(p, _):
        first = jnp.int32(ENT)
        second = jnp.int32(ENT)
        for e in range(FORKS):
            hit = fork_ref[0, e] == p
            second = jnp.where(hit & (first < ENT), e + 1, second)
            first = jnp.where(hit & (first == ENT), e + 1, first)
        slot_of[0, p] = first
        slot_of[1, p] = second
        return 0

    loads[2].wait()
    for c in range(chunks):
        gt_buf[c] = g_buf[c * CW:(c + 1) * CW, :].T

    for part in range(1, len(parts)):
        send_part(part)
    loads[4].wait()
    lax.fori_loop(0, 2 * nc, entry_slots, 0)
    for t in range(2):
        for e in range(ENT + 1):
            acc[t, e] = jnp.zeros((BLK, HD), F32)

    def collect(t, part):
        page_arrivals(t, part).wait_recv()
        page_forward(t, part).start()

    def collected(t):
        for part in range(len(parts)):
            page_forward(t, part).wait_recv()

    def select_pages(t, sel, sel_t):
        for e in range(ENT):
            page = pages[t][chip, core] if e == 0 else pages[t][fork_ref[0, e - 1] // 2, lax.rem(fork_ref[0, e - 1], 2)]
            page = page.reshape(BLK, HD)
            sel[e] = page
            sel_t[:, e * BLK:(e + 1) * BLK] = page.T

    last = len(parts) - 1
    for part in range(last):
        collect(0, part)
        collect(1, part)
    collect(0, last)
    collected(0)
    select_pages(0, ksel, kt_sel)
    loads[3].wait()
    loads[5].wait()

    slot_row = lax.broadcasted_iota(jnp.int32, (BLK, CW), 0)
    key_row = slot_head(slot_row // sub) * sub + lax.rem(slot_row, sub)
    col = lax.broadcasted_iota(jnp.int32, (BLK, CW), 1)

    def halves(a):
        return a.reshape(BLK // 8, 8, CW)

    def scores(c, _):
        q_c = q_buf[pl.ds(pl.multiple_of(c * CW, CW), CW), :]
        top = jnp.full((8, CW), NEG, F32)
        for e in range(ENT):
            raw = dot_nt(ksel[e], q_c) * (FACTOR * LOG2E)
            if e == 0:
                seen = key_row <= (col + c * CW) // groups
            else:
                seen = key_row < vis_ref[0, e - 1]
            raw = jnp.where(seen, raw, NEG)
            s_buf[c, e] = raw
            top = jnp.maximum(top, jnp.max(halves(raw), axis=0))
        top = jnp.max(top, axis=0, keepdims=True)
        total = jnp.zeros((8, CW), F32)
        for e in range(ENT):
            expo = jnp.exp2(s_buf[c, e] - top)
            s_buf[c, e] = expo
            total = total + jnp.sum(halves(expo), axis=0)
        delta_buf[c] = jnp.broadcast_to(1.0 / jnp.sum(total, axis=0, keepdims=True), (8, CW))
        return 0

    lax.fori_loop(0, chunks, scores, 0)

    collect(1, last)
    collected(1)
    select_pages(1, vsel, vt_sel)

    def values(c, _):
        rows_c = pl.ds(pl.multiple_of(c * CW, CW), CW)
        g_c = g_buf[rows_c, :]
        inverse = delta_buf[c][:1]
        out_t = jnp.zeros((HD, CW), F32)
        for e in range(ENT):
            w = s_buf[c, e] * inverse
            s_buf[c, e] = w
            w_b = w.astype(BF16)
            out_t = out_t + dot(vt_sel[:, e * BLK:(e + 1) * BLK], w_b)
            acc[1, e] += dot(w_b, g_c)
        out_b = out_t.astype(BF16)
        att_ref[rows_c, :] = out_b.T
        delta = jnp.sum(out_b.astype(F32) * gt_buf[c].astype(F32), axis=0, keepdims=True)
        delta_buf[c] = jnp.broadcast_to(delta, (8, CW))
        return 0

    lax.fori_loop(0, chunks, values, 0)
    store_att = pltpu.make_async_copy(att_ref, att_hbm, io_sem.at[6])
    store_att.start()

    def spot(t, h, a, b):
        dx, dy = (a, b) if (t + h) % 2 == 0 else (b, a)
        return chip_at(dx, dy)

    def size_a(t, h):
        return nx if (t + h) % 2 == 0 else ny

    def size_b(t, h):
        return ny if (t + h) % 2 == 0 else nx

    def far_first(n):
        return sorted(range(1, n), key=lambda d: -ring(d, n))

    def slot_sum(t, h, page):
        part = pl.ds(h * hb, hb)
        return acc[t, slot_of[0, page], part] + acc[t, slot_of[1, page], part]

    def partner_send(t, h, a):
        return remote(dsend.at[t, h, a], prec.at[t, h, a], dd_send.at[0], dd_recv.at[t, h, a], partner, z)

    def first_send(t, h, a):
        to = spot(t, h, a, 0) * 2 + core
        return remote(rsend.at[t, h, a], rrec.at[t, h, a], r1_send.at[0], r1_recv.at[t, h], to, z)

    def second_send(t, h, b):
        to = spot(t, h, 0, b) * 2 + core
        return remote(ssend.at[t, h, b], srec.at[t, h, b], r2_send.at[0], r2_recv.at[t, h], to, z)

    def to_partner(t):
        for h in (1, 0):
            for a in far_first(size_a(t, h)) + [0]:
                for b in range(size_b(t, h)):
                    dsend[t, h, a, b] = slot_sum(t, h, spot(t, h, a, b) * 2 + (1 - core)).astype(BF16)
                partner_send(t, h, a).start()

    def mine(t, h, a, b):
        return slot_sum(t, h, spot(t, h, a, b) * 2 + core) + prec[t, h, a, b].astype(F32)

    def first_step(t, h):
        for a in far_first(size_a(t, h)):
            partner_send(t, h, a).wait_recv()
            for b in range(size_b(t, h)):
                rsend[t, h, a, b] = mine(t, h, a, b).astype(BF16)
            first_send(t, h, a).start()

    def gathered(t, h, b):
        total = mine(t, h, 0, b)
        for a in range(1, size_a(t, h)):
            total = total + rrec[t, h, a, b].astype(F32)
        return total

    def second_step(t, h):
        partner_send(t, h, 0).wait_recv()
        here = rrec.at[t, h, pl.ds(1, size_a(t, h) - 1)]
        remote(here, here, r1_send.at[0], r1_recv.at[t, h], partner, z).wait_recv()
        for b in far_first(size_b(t, h)):
            ssend[t, h, b] = gathered(t, h, b).astype(BF16)
            second_send(t, h, b).start()

    def zb_copy(t, j):
        back = slot_at[(nz - rel[j]) % nz]
        return remote(fin.at[t, j], zrec.at[t, back], zb_send.at[0], zb_recv.at[t], seq, lax.rem(z + rel[j], nz))

    def finish(t, h):
        total = acc[t, 0, h * hb:(h + 1) * hb] + gathered(t, h, 0)
        here = srec.at[t, h, pl.ds(1, size_b(t, h) - 1)]
        remote(here, here, r2_send.at[0], r2_recv.at[t, h], partner, z).wait_recv()
        for b in range(1, size_b(t, h)):
            total = total + srec[t, h, b].astype(F32)
        if t == 0:
            total = total * FACTOR
        fin[t, h * hz:(h + 1) * hz] = total.astype(BF16).reshape(hz, sub, HD)
        for j in range((h + 1) * hz - 1, h * hz - 1, -1):
            if j == 0:
                zrec[t, 0] = fin[t, 0]
            else:
                zb_copy(t, j).start()

    def result(t, out_ref):
        here = zrec.at[t, pl.ds(1, nz - 1)]
        remote(here, here, zb_send.at[0], zb_recv.at[t], seq, lax.rem(z + 1, nz)).wait_recv()
        out_ref[...] = dot(from_slots, zrec[t].reshape(BLK, HD)).astype(BF16)

    def grads(c, _):
        rows_c = pl.ds(pl.multiple_of(c * CW, CW), CW)
        g_c = g_buf[rows_c, :]
        q_c = q_buf[rows_c, :]
        delta = delta_buf[c][:1]
        dq_t = jnp.zeros((HD, CW), F32)
        for e in range(ENT):
            ds = (s_buf[c, e] * (dot_nt(vsel[e], g_c) - delta)).astype(BF16)
            dq_t = dq_t + dot(kt_sel[:, e * BLK:(e + 1) * BLK], ds)
            acc[0, e] += dot(ds, q_c)
        qg_ref[rows_c, :] = (dq_t * FACTOR).T.astype(BF16)
        return 0

    to_partner(1)
    lax.fori_loop(0, chunks // 2, grads, 0)
    first_step(1, 1)
    first_step(1, 0)
    lax.fori_loop(chunks // 2, chunks, grads, 0)
    store_qg = pltpu.make_async_copy(qg_ref, qg_hbm, io_sem.at[7])
    store_qg.start()
    to_partner(0)
    second_step(1, 1)
    second_step(1, 0)
    first_step(0, 1)
    first_step(0, 0)
    finish(1, 1)
    finish(1, 0)
    second_step(0, 1)
    second_step(0, 0)
    finish(0, 1)
    finish(0, 0)
    result(1, vg_ref)
    result(0, kg_ref)

    store_att.wait()
    store_qg.wait()
    def sent(ref, sem):
        remote(ref, ref, sem, r2_recv.at[0, 0], partner, z).wait_send()

    sent(zsrc.at[:, pl.ds(1, nz - 1)], z_send.at[0])
    sent(dsend, dd_send.at[0])
    sent(rsend.at[:, :, pl.ds(1, nx - 1)], r1_send.at[0])
    sent(ssend.at[:, :, pl.ds(1, nx - 1)], r2_send.at[0])
    sent(fin.at[:, pl.ds(1, nz - 1)], zb_send.at[0])
    for t in range(2):
        sent(pages[t].at[pl.ds(0, nc - 1), 0], ag_send.at[t])
        sent(pages[t].at[:, 0], fw_send.at[t])


def emit(*refs):
    n = (len(refs) - 2) // 3
    sems_in, sems_out = refs[-2:]
    reads = [pltpu.make_async_copy(refs[i], refs[2 * n + i], sems_in.at[i]) for i in range(n)]
    writes = [pltpu.make_async_copy(refs[2 * n + i], refs[n + i], sems_out.at[i]) for i in range(n)]
    for read in reads:
        read.start()
    for read, write in zip(reads, writes):
        read.wait()
        write.start()
    for write in writes:
        write.wait()


def per_device(nx, ny, nz, queries, key_store, value_store, upstream, fork_pages, fork_visible):
    groups = queries.shape[1]
    rows = BLK * groups
    chunks = rows // CW
    nc = nx * ny
    sub = BLK // nz
    hb = BLK // 2
    nm = max(nx, ny)
    dma = pltpu.SemaphoreType.DMA
    vmem = pl.BlockSpec(memory_space=pltpu.VMEM)
    hbm = pl.BlockSpec(memory_space=pltpu.HBM)
    big = jax.ShapeDtypeStruct((rows, HD), BF16)
    small = jax.ShapeDtypeStruct((BLK, HD), BF16)
    outs = (big, big, small, small)
    results = pl.pallas_call(
        functools.partial(kernel, nx, ny, nz, groups),
        out_shape=outs,
        in_specs=[hbm] * 6,
        out_specs=(hbm, hbm, vmem, vmem),
        scratch_shapes=[
            pltpu.VMEM((rows, HD), BF16),
            pltpu.VMEM((rows, HD), BF16),
            pltpu.VMEM((2, BLK, HD), BF16),
            pltpu.VMEM((rows, HD), BF16),
            pltpu.VMEM((rows, HD), BF16),
            pltpu.VMEM((chunks, HD, CW), BF16),
            pltpu.VMEM((chunks, 8, CW), F32),
            pltpu.VMEM((2, nz, sub, HD), BF16),
            pltpu.VMEM((nc, 2, nz, sub, HD), BF16),
            pltpu.VMEM((nc, 2, nz, sub, HD), BF16),
            pltpu.VMEM((ENT, BLK, HD), BF16),
            pltpu.VMEM((ENT, BLK, HD), BF16),
            pltpu.VMEM((HD, ENT * BLK), BF16),
            pltpu.VMEM((HD, ENT * BLK), BF16),
            pltpu.VMEM((chunks, ENT, BLK, CW), F32),
            pltpu.VMEM((2, ENT + 1, BLK, HD), F32),
            pltpu.SMEM((1, FORKS), jnp.int32),
            pltpu.SMEM((1, FORKS), jnp.int32),
            pltpu.SMEM((2, 2 * nc), jnp.int32),
            pltpu.VMEM((2, 2, nm, nm, hb, HD), BF16),
            pltpu.VMEM((2, 2, nm, nm, hb, HD), BF16),
            pltpu.VMEM((2, 2, nm, nm, hb, HD), BF16),
            pltpu.VMEM((2, 2, nm, nm, hb, HD), BF16),
            pltpu.VMEM((2, 2, nm, hb, HD), BF16),
            pltpu.VMEM((2, 2, nm, hb, HD), BF16),
            pltpu.VMEM((2, nz, sub, HD), BF16),
            pltpu.VMEM((2, nz, sub, HD), BF16),
            dma((8,)),
            dma((1,)), dma((2, 4)),
            dma((2,)), dma((2, 4)),
            dma((2,)), dma((2, 4)),
            dma((1,)), dma((2, 2, nm)),
            dma((1,)), dma((2, 2)),
            dma((1,)), dma((2, 2)),
            dma((1,)), dma((2,)),
        ],
        compiler_params=pltpu.CompilerParams(
            collective_id=0, has_side_effects=True
        ),
    )(
        fork_pages, fork_visible,
        key_store.reshape(BLK, HD), value_store.reshape(BLK, HD),
        queries.reshape(rows, HD), upstream.reshape(rows, HD),
    )
    att, qg, kg, vg = pl.pallas_call(
        emit,
        out_shape=outs,
        in_specs=[hbm] * 4,
        out_specs=(hbm,) * 4,
        scratch_shapes=[pltpu.VMEM(o.shape, BF16) for o in outs] + [dma((4,)), dma((4,))],
    )(*results)
    return (
        att.reshape(queries.shape), qg.reshape(queries.shape),
        kg.reshape(key_store.shape), vg.reshape(value_store.shape),
    )


def solution(mesh):
    nc = mesh.shape["seq"] // 2
    nx = 1
    while nx * nx < nc:
        nx *= 2
    placed = (
        P("seq", "head", None),
        P(("seq", "head"), None, None),
        P(("seq", "head"), None, None),
        P("seq", "head", None),
        P("seq", None),
        P("seq", None),
    )
    return jax.shard_map(
        functools.partial(per_device, nx, nc // nx, mesh.shape["head"]),
        mesh=mesh,
        in_specs=placed,
        out_specs=(
            P("seq", "head", None),
            P("seq", "head", None),
            P(("seq", "head"), None, None),
            P(("seq", "head"), None, None),
        ),
        check_vma=False,
    )
```

```python
import functools
import math

import jax
import jax.numpy as jnp
from jax import lax
from jax.experimental import pallas as pl
from jax.experimental.pallas import tpu as pltpu
from jax.sharding import PartitionSpec as P

HD = 128
BLK = 128
FORKS = 8
ENT = FORKS + 1
CW = 256
F32 = jnp.float32
BF16 = jnp.bfloat16
MESH = pl.DeviceIdType.MESH
NT = (((1,), (1,)), ((), ()))
FACTOR = 1.0 / math.sqrt(HD)
LOG2E = 1.4426950408889634
NEG = -1e30


def dot(a, b):
    return jnp.dot(a, b, preferred_element_type=F32)


def dot_nt(a, b):
    return lax.dot_general(a, b, NT, preferred_element_type=F32)


def remote(src, dst, send_sem, recv_sem, seq, head):
    return pltpu.make_async_remote_copy(
        src_ref=src, dst_ref=dst, send_sem=send_sem, recv_sem=recv_sem,
        device_id=(seq, head), device_id_type=MESH,
    )


def kernel(
    nx, ny, nz, groups,
    fork_hbm, vis_hbm, k_hbm, v_hbm, q_hbm, g_hbm,
    att_ref, qg_ref, kg_ref, vg_ref,
    kv_in, q_buf, g_buf, gt_buf, delta_buf,
    zsrc, kpages, vpages, ksel, vsel, kt_sel, vt_sel, s_buf, ds_buf,
    acc, fork_ref, vis_ref, slot_of, dsend, prec, rsend, rrec, ssend, srec, fin, zrec,
    io_sem, z_send, z_recv, la_send, la_recv, pa_send, pa_recv, fw_send, fw_recv,
    dd_send, dd_recv, r1_send, r1_recv, r2_send, r2_recv, zb_send, zb_recv,
):
    nc = nx * ny
    rows = BLK * groups
    chunks = rows // CW
    sub = BLK // nz
    hb = BLK // 2
    hz = nz // 2
    seq = lax.axis_index("seq")
    z = lax.axis_index("head")
    core = lax.rem(seq, 2)
    chip = seq // 2
    x = lax.rem(chip, nx)
    y = chip // nx
    partner = chip * 2 + (1 - core)

    def ring(d, n):
        return min(d, n - d)

    def far_first(n):
        return sorted(range(1, n), key=lambda d: -ring(d, n))

    rel = [(j + 1) // 2 if j % 2 else (nz - j // 2) % nz for j in range(nz)]
    slot_at = {r: j for j, r in enumerate(rel)}
    bounds = [0, 1, 3, 5, 8] if nz == 8 else [0, 1, nz]
    parts = list(zip(bounds[:-1], bounds[1:]))
    part_of = [p for p, (lo, hi) in enumerate(parts) for _ in range(lo, hi)]

    def chip_at(dx, dy):
        return lax.rem(y + dy, ny) * nx + lax.rem(x + dx, nx)

    loads = [
        pltpu.make_async_copy(k_hbm, kv_in.at[0], io_sem.at[0]),
        pltpu.make_async_copy(v_hbm, kv_in.at[1], io_sem.at[1]),
        pltpu.make_async_copy(g_hbm, g_buf, io_sem.at[2]),
        pltpu.make_async_copy(q_hbm, q_buf, io_sem.at[3]),
        pltpu.make_async_copy(fork_hbm, fork_ref, io_sem.at[4]),
        pltpu.make_async_copy(vis_hbm, vis_ref, io_sem.at[5]),
    ]
    barrier = pltpu.get_barrier_semaphore()
    for o in range(1, nz):
        pl.semaphore_signal(barrier, inc=1, device_id=(seq, lax.rem(z + o, nz)), device_id_type=MESH)
    for d in far_first(nx):
        pl.semaphore_signal(barrier, inc=1, device_id=(chip_at(d, 0) * 2 + core, z), device_id_type=MESH)
    for d in far_first(ny):
        pl.semaphore_signal(barrier, inc=1, device_id=(chip_at(0, d) * 2 + core, z), device_id_type=MESH)
    pl.semaphore_signal(barrier, inc=1, device_id=(partner, z), device_id_type=MESH)
    for load in loads:
        load.start()

    r0 = lax.broadcasted_iota(jnp.int32, (BLK, BLK), 0)
    r1 = lax.broadcasted_iota(jnp.int32, (BLK, BLK), 1)

    def slot_head(j):
        return lax.rem(z + jnp.where(lax.rem(j, 2) == 1, (j + 1) // 2, nz - j // 2), nz)

    to_heads = (r1 == lax.rem(r0, sub) * nz + r0 // sub).astype(BF16)
    from_slots = (lax.rem(r0, nz) == slot_head(r1 // sub)) & (r0 // nz == lax.rem(r1, sub))
    from_slots = from_slots.astype(F32).astype(BF16)
    pages = (kpages, vpages)
    for t in range(2):
        loads[t].wait()
        zsrc[t] = dot(to_heads, kv_in[t]).astype(BF16).reshape(nz, sub, HD)
        pages[t][y, x, core, 0] = zsrc[t, z]

    pl.semaphore_wait(barrier, nz - 1 + nx - 1 + ny - 1 + 1)

    def z_copy(t, o):
        head = lax.rem(z + o, nz)
        dst = pages[t].at[y, x, core, slot_at[(nz - o) % nz]]
        return remote(zsrc.at[t, head], dst, z_send.at[0], z_recv.at[t, part_of[slot_at[(nz - o) % nz]]], seq, head)

    def x_first(t, k):
        return (t + k) % 2 == 0

    def spot(t, k, a, b):
        return chip_at(a, b) if x_first(t, k) else chip_at(b, a)

    def size_a(t, k):
        return nx if x_first(t, k) else ny

    def size_b(t, k):
        return ny if x_first(t, k) else nx

    def own_part(t, part):
        lo, hi = parts[part]
        return pages[t].at[y, x, core, pl.ds(lo, hi - lo)]

    def line_send(t, part, d):
        ref = own_part(t, part)
        return remote(ref, ref, la_send.at[t], la_recv.at[t, part], spot(t, part, d, 0) * 2 + core, z)

    def line_arrivals(t, part):
        lo, hi = parts[part]
        ref = pages[t].at[0, pl.ds(0, size_a(t, part) - 1), 0, pl.ds(lo, hi - lo)]
        return remote(ref, ref, la_send.at[t], la_recv.at[t, part], partner, z)

    def plane_send(t, part, d):
        lo, hi = parts[part]
        if x_first(t, part):
            ref = pages[t].at[y, pl.ds(0, nx), core, pl.ds(lo, hi - lo)]
        else:
            ref = pages[t].at[pl.ds(0, ny), x, core, pl.ds(lo, hi - lo)]
        return remote(ref, ref, pa_send.at[t], pa_recv.at[t, part], spot(t, part, 0, d) * 2 + core, z)

    def plane_arrivals(t, part):
        lo, hi = parts[part]
        ref = pages[t].at[pl.ds(0, ny - 1), pl.ds(0, nx), 0, pl.ds(lo, hi - lo)]
        return remote(ref, ref, pa_send.at[t], pa_recv.at[t, part], partner, z)

    def page_forward(t, part):
        lo, hi = parts[part]
        ref = pages[t].at[pl.ds(0, ny), pl.ds(0, nx), core, pl.ds(lo, hi - lo)]
        return remote(ref, ref, fw_send.at[t], fw_recv.at[t, part], partner, z)

    z_order = sorted(range(1, nz), key=lambda o: -ring(o, nz))
    for o in z_order:
        for t in range(2):
            z_copy(t, o).start()

    def send_part(part):
        for t in range(2):
            if part:
                here = own_part(t, part)
                remote(here, here, z_send.at[0], z_recv.at[t, part], seq, lax.rem(z + 1, nz)).wait_recv()
            for d in far_first(size_a(t, part)):
                line_send(t, part, d).start()

    def relay(part):
        for t in range(2):
            line_arrivals(t, part).wait_recv()
            for d in far_first(size_b(t, part)):
                plane_send(t, part, d).start()

    send_part(0)

    def entry_slots(p, _):
        first = jnp.int32(ENT)
        second = jnp.int32(ENT)
        for e in range(FORKS):
            hit = fork_ref[0, e] == p
            second = jnp.where(hit & (first < ENT), e + 1, second)
            first = jnp.where(hit & (first == ENT), e + 1, first)
        slot_of[0, p] = first
        slot_of[1, p] = second
        return 0

    loads[2].wait()
    for c in range(chunks):
        gt_buf[c] = g_buf[c * CW:(c + 1) * CW, :].T

    for part in range(1, len(parts)):
        send_part(part)
        if part > 1:
            relay(part - 2)
    for part in range(max(0, len(parts) - 2), len(parts)):
        relay(part)
    loads[4].wait()
    lax.fori_loop(0, 2 * nc, entry_slots, 0)
    for t in range(2):
        for e in range(ENT + 1):
            acc[t, e] = jnp.zeros((BLK, HD), F32)

    def collect(t, part):
        plane_arrivals(t, part).wait_recv()
        page_forward(t, part).start()

    def collected(t):
        for part in range(len(parts)):
            page_forward(t, part).wait_recv()

    def page_at(p):
        return p // (2 * nx), lax.rem(p // 2, nx), lax.rem(p, 2)

    def select_pages(t, sel, sel_t):
        for e in range(ENT):
            page = pages[t][y, x, core] if e == 0 else pages[t][page_at(fork_ref[0, e - 1])]
            page = page.reshape(BLK, HD)
            sel[e] = page
            sel_t[:, e * BLK:(e + 1) * BLK] = page.T

    last = len(parts) - 1
    for part in range(last):
        collect(0, part)
        collect(1, part)
    collect(0, last)
    collected(0)
    select_pages(0, ksel, kt_sel)
    loads[3].wait()
    loads[5].wait()

    slot_row = lax.broadcasted_iota(jnp.int32, (BLK, CW), 0)
    key_row = slot_head(slot_row // sub) * sub + lax.rem(slot_row, sub)
    col = lax.broadcasted_iota(jnp.int32, (BLK, CW), 1)

    def halves(a):
        return a.reshape(BLK // 8, 8, CW)

    def scores(c, _):
        q_c = q_buf[pl.ds(pl.multiple_of(c * CW, CW), CW), :]
        top = jnp.full((8, CW), NEG, F32)
        for e in range(ENT):
            raw = dot_nt(ksel[e], q_c) * (FACTOR * LOG2E)
            if e == 0:
                seen = key_row <= (col + c * CW) // groups
            else:
                seen = key_row < vis_ref[0, e - 1]
            raw = jnp.where(seen, raw, NEG)
            s_buf[c, e] = raw
            top = jnp.maximum(top, jnp.max(halves(raw), axis=0))
        top = jnp.max(top, axis=0, keepdims=True)
        total = jnp.zeros((8, CW), F32)
        for e in range(ENT):
            expo = jnp.exp2(s_buf[c, e] - top)
            s_buf[c, e] = expo
            total = total + jnp.sum(halves(expo), axis=0)
        delta_buf[c] = jnp.broadcast_to(1.0 / jnp.sum(total, axis=0, keepdims=True), (8, CW))
        return 0

    lax.fori_loop(0, chunks, scores, 0)

    collect(1, last)
    collected(1)
    select_pages(1, vsel, vt_sel)

    def values(c, _):
        rows_c = pl.ds(pl.multiple_of(c * CW, CW), CW)
        g_c = g_buf[rows_c, :]
        inverse = delta_buf[c][:1]
        out_t = jnp.zeros((HD, CW), F32)
        for e in range(ENT):
            w = s_buf[c, e] * inverse
            s_buf[c, e] = w
            w_b = w.astype(BF16)
            out_t = out_t + dot(vt_sel[:, e * BLK:(e + 1) * BLK], w_b)
            acc[1, e] += dot(w_b, g_c)
        out_b = out_t.astype(BF16)
        att_ref[rows_c, :] = out_b.T
        delta = jnp.sum(out_b.astype(F32) * gt_buf[c].astype(F32), axis=0, keepdims=True)
        delta_buf[c] = jnp.broadcast_to(delta, (8, CW))
        return 0

    lax.fori_loop(0, chunks, values, 0)

    def slot_sum(t, h, page):
        part = pl.ds(h * hb, hb)
        return acc[t, slot_of[0, page], part] + acc[t, slot_of[1, page], part]

    def partner_send(t, h, a):
        return remote(dsend.at[t, h, a], prec.at[t, h, a], dd_send.at[0], dd_recv.at[t, h, a], partner, z)

    def first_send(t, h, a):
        to = spot(t, h, a, 0) * 2 + core
        return remote(rsend.at[t, h, a], rrec.at[t, h, a], r1_send.at[0], r1_recv.at[t, h], to, z)

    def second_send(t, h, b):
        to = spot(t, h, 0, b) * 2 + core
        return remote(ssend.at[t, h, b], srec.at[t, h, b], r2_send.at[0], r2_recv.at[t, h], to, z)

    def to_partner(t):
        for h in (1, 0):
            for a in far_first(size_a(t, h)) + [0]:
                for b in range(size_b(t, h)):
                    dsend[t, h, a, b] = slot_sum(t, h, spot(t, h, a, b) * 2 + (1 - core)).astype(BF16)
                partner_send(t, h, a).start()

    def mine(t, h, a, b):
        return slot_sum(t, h, spot(t, h, a, b) * 2 + core) + prec[t, h, a, b].astype(F32)

    def first_step(t, h):
        for a in far_first(size_a(t, h)):
            partner_send(t, h, a).wait_recv()
            for b in range(size_b(t, h)):
                rsend[t, h, a, b] = mine(t, h, a, b).astype(BF16)
            first_send(t, h, a).start()

    def gathered(t, h, b):
        total = mine(t, h, 0, b)
        for a in range(1, size_a(t, h)):
            total = total + rrec[t, h, a, b].astype(F32)
        return total

    def second_step(t, h):
        partner_send(t, h, 0).wait_recv()
        here = rrec.at[t, h, pl.ds(1, size_a(t, h) - 1)]
        remote(here, here, r1_send.at[0], r1_recv.at[t, h], partner, z).wait_recv()
        for b in far_first(size_b(t, h)):
            ssend[t, h, b] = gathered(t, h, b).astype(BF16)
            second_send(t, h, b).start()

    def zb_copy(t, j):
        back = slot_at[(nz - rel[j]) % nz]
        return remote(fin.at[t, j], zrec.at[t, back], zb_send.at[0], zb_recv.at[t], seq, lax.rem(z + rel[j], nz))

    def finish(t, h):
        total = acc[t, 0, h * hb:(h + 1) * hb] + gathered(t, h, 0)
        here = srec.at[t, h, pl.ds(1, size_b(t, h) - 1)]
        remote(here, here, r2_send.at[0], r2_recv.at[t, h], partner, z).wait_recv()
        for b in range(1, size_b(t, h)):
            total = total + srec[t, h, b].astype(F32)
        if t == 0:
            total = total * FACTOR
        fin[t, h * hz:(h + 1) * hz] = total.astype(BF16).reshape(hz, sub, HD)
        for j in range((h + 1) * hz - 1, h * hz - 1, -1):
            if j == 0:
                zrec[t, 0] = fin[t, 0]
            else:
                zb_copy(t, j).start()

    def result(t, out_ref):
        here = zrec.at[t, pl.ds(1, nz - 1)]
        remote(here, here, zb_send.at[0], zb_recv.at[t], seq, lax.rem(z + 1, nz)).wait_recv()
        out_ref[...] = dot(from_slots, zrec[t].reshape(BLK, HD)).astype(BF16)

    def grads(c, _):
        rows_c = pl.ds(pl.multiple_of(c * CW, CW), CW)
        g_c = g_buf[rows_c, :]
        q_c = q_buf[rows_c, :]
        delta = delta_buf[c][:1]
        for e in range(ENT):
            ds = (s_buf[c, e] * (dot_nt(vsel[e], g_c) - delta)).astype(BF16)
            ds_buf[c, e * BLK:(e + 1) * BLK, :] = ds
            acc[0, e] += dot(ds, q_c)
        return 0

    def query_grads(c, _):
        rows_c = pl.ds(pl.multiple_of(c * CW, CW), CW)
        dq_t = dot(kt_sel[...], ds_buf[c])
        qg_ref[rows_c, :] = (dq_t * FACTOR).T.astype(BF16)
        return 0

    to_partner(1)
    lax.fori_loop(0, chunks // 2, grads, 0)
    first_step(1, 1)
    first_step(1, 0)
    lax.fori_loop(chunks // 2, chunks, grads, 0)
    to_partner(0)
    lax.fori_loop(0, chunks, query_grads, 0)
    second_step(1, 1)
    second_step(1, 0)
    first_step(0, 1)
    first_step(0, 0)
    finish(1, 1)
    finish(1, 0)
    second_step(0, 1)
    second_step(0, 0)
    finish(0, 1)
    finish(0, 0)
    result(1, vg_ref)
    result(0, kg_ref)


    def sent(ref, sem):
        remote(ref, ref, sem, r2_recv.at[0, 0], partner, z).wait_send()

    sent(zsrc.at[:, pl.ds(1, nz - 1)], z_send.at[0])
    sent(dsend, dd_send.at[0])
    sent(rsend.at[:, :, pl.ds(1, nx - 1)], r1_send.at[0])
    sent(ssend.at[:, :, pl.ds(1, nx - 1)], r2_send.at[0])
    sent(fin.at[:, pl.ds(1, nz - 1)], zb_send.at[0])
    for t in range(2):
        sent(pages[t].at[0, pl.ds(0, nx - 1), 0], la_send.at[t])
        sent(pages[t].at[pl.ds(0, ny - 1), :, 0], pa_send.at[t])
        sent(pages[t].at[:, :, 0], fw_send.at[t])


def emit(*refs):
    n = (len(refs) - 1) // 2
    copies = [pltpu.make_async_copy(refs[i], refs[n + i], refs[-1].at[i]) for i in range(n)]
    for copy in copies:
        copy.start()
    for copy in copies:
        copy.wait()


def per_device(nx, ny, nz, queries, key_store, value_store, upstream, fork_pages, fork_visible):
    groups = queries.shape[1]
    rows = BLK * groups
    chunks = rows // CW
    nc = nx * ny
    sub = BLK // nz
    hb = BLK // 2
    nm = max(nx, ny)
    dma = pltpu.SemaphoreType.DMA
    vmem = pl.BlockSpec(memory_space=pltpu.VMEM)
    hbm = pl.BlockSpec(memory_space=pltpu.HBM)
    big = jax.ShapeDtypeStruct((rows, HD), BF16)
    small = jax.ShapeDtypeStruct((BLK, HD), BF16)
    outs = (big, big, small, small)
    results = pl.pallas_call(
        functools.partial(kernel, nx, ny, nz, groups),
        out_shape=tuple(pltpu.VMEM(o.shape, BF16) for o in outs),
        in_specs=[hbm] * 6,
        out_specs=(vmem,) * 4,
        scratch_shapes=[
            pltpu.VMEM((2, BLK, HD), BF16),
            pltpu.VMEM((rows, HD), BF16),
            pltpu.VMEM((rows, HD), BF16),
            pltpu.VMEM((chunks, HD, CW), BF16),
            pltpu.VMEM((chunks, 8, CW), F32),
            pltpu.VMEM((2, nz, sub, HD), BF16),
            pltpu.VMEM((ny, nx, 2, nz, sub, HD), BF16),
            pltpu.VMEM((ny, nx, 2, nz, sub, HD), BF16),
            pltpu.VMEM((ENT, BLK, HD), BF16),
            pltpu.VMEM((ENT, BLK, HD), BF16),
            pltpu.VMEM((HD, ENT * BLK), BF16),
            pltpu.VMEM((HD, ENT * BLK), BF16),
            pltpu.VMEM((chunks, ENT, BLK, CW), F32),
            pltpu.VMEM((chunks, ENT * BLK, CW), BF16),
            pltpu.VMEM((2, ENT + 1, BLK, HD), F32),
            pltpu.SMEM((1, FORKS), jnp.int32),
            pltpu.SMEM((1, FORKS), jnp.int32),
            pltpu.SMEM((2, 2 * nc), jnp.int32),
            pltpu.VMEM((2, 2, nm, nm, hb, HD), BF16),
            pltpu.VMEM((2, 2, nm, nm, hb, HD), BF16),
            pltpu.VMEM((2, 2, nm, nm, hb, HD), BF16),
            pltpu.VMEM((2, 2, nm, nm, hb, HD), BF16),
            pltpu.VMEM((2, 2, nm, hb, HD), BF16),
            pltpu.VMEM((2, 2, nm, hb, HD), BF16),
            pltpu.VMEM((2, nz, sub, HD), BF16),
            pltpu.VMEM((2, nz, sub, HD), BF16),
            dma((6,)),
            dma((1,)), dma((2, 4)),
            dma((2,)), dma((2, 4)),
            dma((2,)), dma((2, 4)),
            dma((2,)), dma((2, 4)),
            dma((1,)), dma((2, 2, nm)),
            dma((1,)), dma((2, 2)),
            dma((1,)), dma((2, 2)),
            dma((1,)), dma((2,)),
        ],
        compiler_params=pltpu.CompilerParams(
            collective_id=0, has_side_effects=True
        ),
    )(
        fork_pages, fork_visible,
        key_store.reshape(BLK, HD), value_store.reshape(BLK, HD),
        queries.reshape(rows, HD), upstream.reshape(rows, HD),
    )
    att, qg, kg, vg = pl.pallas_call(
        emit,
        out_shape=outs,
        in_specs=[vmem] * 4,
        out_specs=(hbm,) * 4,
        scratch_shapes=[dma((4,))],
        compiler_params=pltpu.CompilerParams(vmem_limit_bytes=4 * 2**20),
    )(*results)
    return (
        att.reshape(queries.shape), qg.reshape(queries.shape),
        kg.reshape(key_store.shape), vg.reshape(value_store.shape),
    )


def solution(mesh):
    nc = mesh.shape["seq"] // 2
    nx = 1
    while nx * nx < nc:
        nx *= 2
    placed = (
        P("seq", "head", None),
        P(("seq", "head"), None, None),
        P(("seq", "head"), None, None),
        P("seq", "head", None),
        P("seq", None),
        P("seq", None),
    )
    return jax.shard_map(
        functools.partial(per_device, nx, nc // nx, mesh.shape["head"]),
        mesh=mesh,
        in_specs=placed,
        out_specs=(
            P("seq", "head", None),
            P("seq", "head", None),
            P(("seq", "head"), None, None),
            P(("seq", "head"), None, None),
        ),
        check_vma=False,
    )
```

```python
import functools
import math

import jax
import jax.numpy as jnp
from jax import lax
from jax.experimental import pallas as pl
from jax.experimental.pallas import tpu as pltpu
from jax.sharding import PartitionSpec as P

HD = 128
BLK = 128
FORKS = 8
ENT = FORKS + 1
CW = 256
F32 = jnp.float32
BF16 = jnp.bfloat16
MESH = pl.DeviceIdType.MESH
NT = (((1,), (1,)), ((), ()))
FACTOR = 1.0 / math.sqrt(HD)
LOG2E = 1.4426950408889634
NEG = -1e30


def dot(a, b):
    return jnp.dot(a, b, preferred_element_type=F32)


def dot_nt(a, b):
    return lax.dot_general(a, b, NT, preferred_element_type=F32)


def remote(src, dst, send_sem, recv_sem, seq, head):
    return pltpu.make_async_remote_copy(
        src_ref=src, dst_ref=dst, send_sem=send_sem, recv_sem=recv_sem,
        device_id=(seq, head), device_id_type=MESH,
    )


def kernel(
    nx, ny, nz, groups,
    fork_hbm, vis_hbm, k_hbm, v_hbm, q_hbm, g_hbm,
    att_ref, qg_ref, kg_ref, vg_ref,
    kv_in, q_buf, g_buf, gt_buf, delta_buf, top_buf, sum_buf,
    zsrc, knear, kfar, vnear, vfar, ksel, vsel, kt_sel, vt_sel, s_buf, ds_buf,
    acc, fork_ref, vis_ref, slot_of, dsend, prec, rsend, rrec, ssend, srec, fin, zrec,
    io_sem, z_send, z_recv, la_send, la_recv, pa_send, pa_recv, fw_send, fw_recv,
    dd_send, dd_recv, r1_send, r1_recv, r2_send, r2_recv, zb_send, zb_recv,
):
    nc = nx * ny
    rows = BLK * groups
    chunks = rows // CW
    sub = BLK // nz
    hb = BLK // 2
    hz = nz // 2
    seq = lax.axis_index("seq")
    z = lax.axis_index("head")
    core = lax.rem(seq, 2)
    chip = seq // 2
    x = lax.rem(chip, nx)
    y = chip // nx
    partner = chip * 2 + (1 - core)

    def ring(d, n):
        return min(d, n - d)

    def far_first(n):
        return sorted(range(1, n), key=lambda d: -ring(d, n))

    rel = [(j + 1) // 2 if j % 2 else (nz - j // 2) % nz for j in range(nz)]
    slot_at = {r: j for j, r in enumerate(rel)}
    bounds = [0, 1, 3, 4, 5, 8] if nz == 8 else [0, 1, nz]
    parts = list(zip(bounds[:-1], bounds[1:]))
    part_of = [p for p, (lo, hi) in enumerate(parts) for _ in range(lo, hi)]

    def chip_at(dx, dy):
        return lax.rem(y + dy, ny) * nx + lax.rem(x + dx, nx)

    loads = [
        pltpu.make_async_copy(k_hbm, kv_in.at[0], io_sem.at[0]),
        pltpu.make_async_copy(v_hbm, kv_in.at[1], io_sem.at[1]),
        pltpu.make_async_copy(g_hbm, g_buf, io_sem.at[2]),
        pltpu.make_async_copy(q_hbm, q_buf, io_sem.at[3]),
        pltpu.make_async_copy(fork_hbm, fork_ref, io_sem.at[4]),
        pltpu.make_async_copy(vis_hbm, vis_ref, io_sem.at[5]),
    ]
    barrier = pltpu.get_barrier_semaphore()
    for o in range(1, nz):
        pl.semaphore_signal(barrier, inc=1, device_id=(seq, lax.rem(z + o, nz)), device_id_type=MESH)
    for d in far_first(nx):
        pl.semaphore_signal(barrier, inc=1, device_id=(chip_at(d, 0) * 2 + core, z), device_id_type=MESH)
    for d in far_first(ny):
        pl.semaphore_signal(barrier, inc=1, device_id=(chip_at(0, d) * 2 + core, z), device_id_type=MESH)
    pl.semaphore_signal(barrier, inc=1, device_id=(partner, z), device_id_type=MESH)
    for load in loads:
        load.start()

    r0 = lax.broadcasted_iota(jnp.int32, (BLK, BLK), 0)
    r1 = lax.broadcasted_iota(jnp.int32, (BLK, BLK), 1)

    def slot_head(j):
        return lax.rem(z + jnp.where(lax.rem(j, 2) == 1, (j + 1) // 2, nz - j // 2), nz)

    to_heads = (r1 == lax.rem(r0, sub) * nz + r0 // sub).astype(BF16)
    from_slots = (lax.rem(r0, nz) == slot_head(r1 // sub)) & (r0 // nz == lax.rem(r1, sub))
    from_slots = from_slots.astype(F32).astype(BF16)
    pages = ((knear, kfar), (vnear, vfar))
    for t in range(2):
        loads[t].wait()
        zsrc[t] = dot(to_heads, kv_in[t]).astype(BF16).reshape(nz, sub, HD)
        pages[t][0][y, x, core, 0] = zsrc[t, z]

    pl.semaphore_wait(barrier, nz - 1 + nx - 1 + ny - 1 + 1)

    def z_copy(t, o):
        head = lax.rem(z + o, nz)
        j = slot_at[(nz - o) % nz]
        dst = pages[t][j // hz].at[y, x, core, j % hz]
        return remote(zsrc.at[t, head], dst, z_send.at[0], z_recv.at[t, part_of[j]], seq, head)

    def x_first(t, k):
        return (t + k) % 2 == 0

    def spot(t, k, a, b):
        return chip_at(a, b) if x_first(t, k) else chip_at(b, a)

    def size_a(t, k):
        return nx if x_first(t, k) else ny

    def size_b(t, k):
        return ny if x_first(t, k) else nx

    def part_of_pages(t, part, ys, xs, cs):
        lo, hi = parts[part]
        return pages[t][lo // hz].at[ys, xs, cs, pl.ds(lo % hz, hi - lo)]

    def own_part(t, part):
        return part_of_pages(t, part, y, x, core)

    def line_send(t, part, d):
        ref = own_part(t, part)
        return remote(ref, ref, la_send.at[t], la_recv.at[t, part], spot(t, part, d, 0) * 2 + core, z)

    def line_arrivals(t, part):
        ref = part_of_pages(t, part, 0, pl.ds(0, size_a(t, part) - 1), 0)
        return remote(ref, ref, la_send.at[t], la_recv.at[t, part], partner, z)

    def plane_send(t, part, d):
        if x_first(t, part):
            ref = part_of_pages(t, part, y, pl.ds(0, nx), core)
        else:
            ref = part_of_pages(t, part, pl.ds(0, ny), x, core)
        return remote(ref, ref, pa_send.at[t], pa_recv.at[t, part], spot(t, part, 0, d) * 2 + core, z)

    def plane_arrivals(t, part):
        ref = part_of_pages(t, part, pl.ds(0, ny - 1), pl.ds(0, nx), 0)
        return remote(ref, ref, pa_send.at[t], pa_recv.at[t, part], partner, z)

    def page_forward(t, part):
        ref = part_of_pages(t, part, pl.ds(0, ny), pl.ds(0, nx), core)
        return remote(ref, ref, fw_send.at[t], fw_recv.at[t, part], partner, z)

    z_order = sorted(range(1, nz), key=lambda o: -ring(o, nz))
    for o in z_order:
        for t in range(2):
            z_copy(t, o).start()

    def send_part(part):
        for t in range(2):
            if part:
                here = own_part(t, part)
                remote(here, here, z_send.at[0], z_recv.at[t, part], seq, lax.rem(z + 1, nz)).wait_recv()
            for d in far_first(size_a(t, part)):
                line_send(t, part, d).start()

    def relay(part):
        for t in range(2):
            line_arrivals(t, part).wait_recv()
            for d in far_first(size_b(t, part)):
                plane_send(t, part, d).start()

    send_part(0)

    def entry_slots(p, _):
        first = jnp.int32(ENT)
        second = jnp.int32(ENT)
        for e in range(FORKS):
            hit = fork_ref[0, e] == p
            second = jnp.where(hit & (first < ENT), e + 1, second)
            first = jnp.where(hit & (first == ENT), e + 1, first)
        slot_of[0, p] = first
        slot_of[1, p] = second
        return 0

    loads[2].wait()
    for c in range(chunks):
        gt_buf[c] = g_buf[c * CW:(c + 1) * CW, :].T

    for part in range(1, len(parts)):
        send_part(part)
        if part > 1:
            relay(part - 2)
    for part in range(max(0, len(parts) - 2), len(parts)):
        relay(part)
    loads[4].wait()
    lax.fori_loop(0, 2 * nc, entry_slots, 0)
    for t in range(2):
        for h in range(2):
            acc[t, h] = jnp.zeros((ENT + 1, hb, HD), F32)

    def collect(t, part):
        plane_arrivals(t, part).wait_recv()
        page_forward(t, part).start()

    def collected(t, which):
        for part in which:
            page_forward(t, part).wait_recv()

    def page_at(p):
        return p // (2 * nx), lax.rem(p // 2, nx), lax.rem(p, 2)

    def select_pages(t, sel, h):
        for e in range(ENT):
            at = (y, x, core) if e == 0 else page_at(fork_ref[0, e - 1])
            page = pages[t][h][at[0], at[1], at[2]]
            sel[h, e * hb:(e + 1) * hb, :] = page.reshape(hb, HD)

    def transposed(sel, sel_t, h):
        for e in range(ENT):
            sel_t[h, :, e * hb:(e + 1) * hb] = sel[h, e * hb:(e + 1) * hb, :].T

    slot_row = lax.broadcasted_iota(jnp.int32, (hb, CW), 0)
    col = lax.broadcasted_iota(jnp.int32, (hb, CW), 1)

    def eights(a):
        return a.reshape(hb // 8, 8, CW)

    def lanes(c):
        return pl.ds(pl.multiple_of(c * CW, CW), CW)

    def scores(h):
        key_row = slot_head(h * hz + slot_row // sub) * sub + lax.rem(slot_row, sub)

        def step(c, _):
            q_c = q_buf[lanes(c), :]
            top = jnp.full((8, CW), NEG, F32)
            for e in range(ENT):
                raw = dot_nt(ksel[h, e * hb:(e + 1) * hb, :], q_c) * (FACTOR * LOG2E)
                if e == 0:
                    seen = key_row <= (col + c * CW) // groups
                else:
                    seen = key_row < vis_ref[0, e - 1]
                raw = jnp.where(seen, raw, NEG)
                s_buf[c, h, e] = raw
                top = jnp.maximum(top, jnp.max(eights(raw), axis=0))
            top = jnp.broadcast_to(jnp.max(top, axis=0, keepdims=True), (8, CW))
            total = jnp.zeros((8, CW), F32)
            for e in range(ENT):
                expo = jnp.exp2(s_buf[c, h, e] - top[:1])
                s_buf[c, h, e] = expo
                total = total + jnp.sum(eights(expo), axis=0)
            top_buf[c, h] = top
            sum_buf[c, h] = jnp.broadcast_to(jnp.sum(total, axis=0, keepdims=True), (8, CW))
            return 0

        lax.fori_loop(0, chunks, step, 0)

    near = range(part_of[hz])
    rest = range(part_of[hz], len(parts))
    for part in near:
        collect(0, part)
        collect(1, part)
    collected(0, near)
    select_pages(0, ksel, 0)
    loads[3].wait()
    loads[5].wait()
    scores(0)
    collected(1, near)
    select_pages(1, vsel, 0)
    transposed(vsel, vt_sel, 0)
    transposed(ksel, kt_sel, 0)
    for part in rest:
        collect(0, part)
        collect(1, part)
    collected(0, rest)
    select_pages(0, ksel, 1)
    scores(1)
    collected(1, rest)
    select_pages(1, vsel, 1)
    transposed(vsel, vt_sel, 1)

    def values(c, _):
        g_c = g_buf[lanes(c), :]
        top = jnp.maximum(top_buf[c, 0], top_buf[c, 1])
        scale = [jnp.exp2(top_buf[c, h] - top) for h in range(2)]
        inverse = 1.0 / (sum_buf[c, 0] * scale[0] + sum_buf[c, 1] * scale[1])
        out_t = jnp.zeros((HD, CW), F32)
        for h in range(2):
            factor = (scale[h] * inverse)[:1]
            for e in range(ENT):
                w = s_buf[c, h, e] * factor
                s_buf[c, h, e] = w
                ds_buf[c, h, e * hb:(e + 1) * hb, :] = w.astype(BF16)
            w_b = ds_buf[c, h]
            acc[1, h, :ENT] += dot(w_b, g_c).reshape(ENT, hb, HD)
            out_t = out_t + dot(vt_sel[h], w_b)
        out_b = out_t.astype(BF16)
        att_ref[lanes(c), :] = out_b.T
        delta = jnp.sum(out_b.astype(F32) * gt_buf[c].astype(F32), axis=0, keepdims=True)
        delta_buf[c] = jnp.broadcast_to(delta, (8, CW))
        return 0

    lax.fori_loop(0, chunks, values, 0)

    def slot_sum(t, h, page):
        return acc[t, h, slot_of[0, page]] + acc[t, h, slot_of[1, page]]

    def partner_send(t, h, a):
        return remote(dsend.at[t, h, a], prec.at[t, h, a], dd_send.at[0], dd_recv.at[t, h, a], partner, z)

    def first_send(t, h, a):
        to = spot(t, h, a, 0) * 2 + core
        return remote(rsend.at[t, h, a], rrec.at[t, h, a], r1_send.at[0], r1_recv.at[t, h], to, z)

    def second_send(t, h, b):
        to = spot(t, h, 0, b) * 2 + core
        return remote(ssend.at[t, h, b], srec.at[t, h, b], r2_send.at[0], r2_recv.at[t, h], to, z)

    def to_partner(t, h):
        for a in far_first(size_a(t, h)) + [0]:
            for b in range(size_b(t, h)):
                dsend[t, h, a, b] = slot_sum(t, h, spot(t, h, a, b) * 2 + (1 - core)).astype(BF16)
            partner_send(t, h, a).start()

    def mine(t, h, a, b):
        return slot_sum(t, h, spot(t, h, a, b) * 2 + core) + prec[t, h, a, b].astype(F32)

    def first_step(t, h, lo=0, hi=None):
        for a in far_first(size_a(t, h))[lo:hi]:
            partner_send(t, h, a).wait_recv()
            for b in range(size_b(t, h)):
                rsend[t, h, a, b] = mine(t, h, a, b).astype(BF16)
            first_send(t, h, a).start()

    def gathered(t, h, b):
        total = mine(t, h, 0, b)
        for a in range(1, size_a(t, h)):
            total = total + rrec[t, h, a, b].astype(F32)
        return total

    def second_step(t, h):
        partner_send(t, h, 0).wait_recv()
        here = rrec.at[t, h, pl.ds(1, size_a(t, h) - 1)]
        remote(here, here, r1_send.at[0], r1_recv.at[t, h], partner, z).wait_recv()
        for b in far_first(size_b(t, h)):
            ssend[t, h, b] = gathered(t, h, b).astype(BF16)
            second_send(t, h, b).start()

    def zb_copy(t, j):
        back = slot_at[(nz - rel[j]) % nz]
        return remote(fin.at[t, j], zrec.at[t, back], zb_send.at[0], zb_recv.at[t], seq, lax.rem(z + rel[j], nz))

    def finish(t, h):
        total = acc[t, h, 0] + gathered(t, h, 0)
        here = srec.at[t, h, pl.ds(1, size_b(t, h) - 1)]
        remote(here, here, r2_send.at[0], r2_recv.at[t, h], partner, z).wait_recv()
        for b in range(1, size_b(t, h)):
            total = total + srec[t, h, b].astype(F32)
        if t == 0:
            total = total * FACTOR
        fin[t, h * hz:(h + 1) * hz] = total.astype(BF16).reshape(hz, sub, HD)
        for j in range((h + 1) * hz - 1, h * hz - 1, -1):
            if j == 0:
                zrec[t, 0] = fin[t, 0]
            else:
                zb_copy(t, j).start()

    def result(t, out_ref):
        here = zrec.at[t, pl.ds(1, nz - 1)]
        remote(here, here, zb_send.at[0], zb_recv.at[t], seq, lax.rem(z + 1, nz)).wait_recv()
        out_ref[...] = dot(from_slots, zrec[t].reshape(BLK, HD)).astype(BF16)

    def grads(h):
        def step(c, _):
            g_c = g_buf[lanes(c), :]
            delta = delta_buf[c][:1]
            for e in range(ENT):
                part = pl.ds(e * hb, hb)
                ds_buf[c, h, part] = (s_buf[c, h, e] * (dot_nt(vsel[h, part], g_c) - delta)).astype(BF16)
            acc[0, h, :ENT] += dot(ds_buf[c, h], q_buf[lanes(c), :]).reshape(ENT, hb, HD)
            return 0

        lax.fori_loop(0, chunks, step, 0)

    def query_grads(c, _):
        dq_t = dot(kt_sel[0], ds_buf[c, 0]) + dot(kt_sel[1], ds_buf[c, 1])
        qg_ref[lanes(c), :] = (dq_t * FACTOR).T.astype(BF16)
        return 0

    to_partner(1, 1)
    to_partner(1, 0)
    grads(1)
    to_partner(0, 1)
    first_step(1, 1)
    first_step(1, 0, 0, 1)
    grads(0)
    to_partner(0, 0)
    first_step(0, 1)
    first_step(1, 0, 1)
    transposed(ksel, kt_sel, 1)
    first_step(0, 0)
    lax.fori_loop(0, chunks, query_grads, 0)
    second_step(1, 1)
    second_step(0, 1)
    second_step(1, 0)
    second_step(0, 0)
    finish(1, 1)
    finish(0, 1)
    finish(1, 0)
    finish(0, 0)
    result(1, vg_ref)
    result(0, kg_ref)


    def sent(ref, sem):
        remote(ref, ref, sem, r2_recv.at[0, 0], partner, z).wait_send()

    sent(zsrc.at[:, pl.ds(1, nz - 1)], z_send.at[0])
    sent(dsend, dd_send.at[0])
    sent(rsend.at[:, :, pl.ds(1, nx - 1)], r1_send.at[0])
    sent(ssend.at[:, :, pl.ds(1, nx - 1)], r2_send.at[0])
    sent(fin.at[:, pl.ds(1, nz - 1)], zb_send.at[0])
    for t in range(2):
        sent(pages[t][0].at[pl.ds(0, nx - 1), pl.ds(0, 2), 0], la_send.at[t])
        sent(pages[t][0].at[pl.ds(0, ny - 1)], pa_send.at[t])
        sent(pages[t][0], fw_send.at[t])


def emit(*refs):
    n = (len(refs) - 1) // 2
    copies = [pltpu.make_async_copy(refs[i], refs[n + i], refs[-1].at[i]) for i in range(n)]
    for copy in copies:
        copy.start()
    for copy in copies:
        copy.wait()


def per_device(nx, ny, nz, queries, key_store, value_store, upstream, fork_pages, fork_visible):
    groups = queries.shape[1]
    rows = BLK * groups
    chunks = rows // CW
    nc = nx * ny
    sub = BLK // nz
    hb = BLK // 2
    nm = max(nx, ny)
    dma = pltpu.SemaphoreType.DMA
    vmem = pl.BlockSpec(memory_space=pltpu.VMEM)
    hbm = pl.BlockSpec(memory_space=pltpu.HBM)
    big = jax.ShapeDtypeStruct((rows, HD), BF16)
    small = jax.ShapeDtypeStruct((BLK, HD), BF16)
    outs = (big, big, small, small)
    results = pl.pallas_call(
        functools.partial(kernel, nx, ny, nz, groups),
        out_shape=tuple(pltpu.VMEM(o.shape, BF16) for o in outs),
        in_specs=[hbm] * 6,
        out_specs=(vmem,) * 4,
        scratch_shapes=[
            pltpu.VMEM((2, BLK, HD), BF16),
            pltpu.VMEM((rows, HD), BF16),
            pltpu.VMEM((rows, HD), BF16),
            pltpu.VMEM((chunks, HD, CW), BF16),
            pltpu.VMEM((chunks, 8, CW), F32),
            pltpu.VMEM((chunks, 2, 8, CW), F32),
            pltpu.VMEM((chunks, 2, 8, CW), F32),
            pltpu.VMEM((2, nz, sub, HD), BF16),
            pltpu.VMEM((ny, nx, 2, nz // 2, sub, HD), BF16),
            pltpu.VMEM((ny, nx, 2, nz // 2, sub, HD), BF16),
            pltpu.VMEM((ny, nx, 2, nz // 2, sub, HD), BF16),
            pltpu.VMEM((ny, nx, 2, nz // 2, sub, HD), BF16),
            pltpu.VMEM((2, ENT * hb, HD), BF16),
            pltpu.VMEM((2, ENT * hb, HD), BF16),
            pltpu.VMEM((2, HD, ENT * hb), BF16),
            pltpu.VMEM((2, HD, ENT * hb), BF16),
            pltpu.VMEM((chunks, 2, ENT, hb, CW), F32),
            pltpu.VMEM((chunks, 2, ENT * hb, CW), BF16),
            pltpu.VMEM((2, 2, ENT + 1, hb, HD), F32),
            pltpu.SMEM((1, FORKS), jnp.int32),
            pltpu.SMEM((1, FORKS), jnp.int32),
            pltpu.SMEM((2, 2 * nc), jnp.int32),
            pltpu.VMEM((2, 2, nm, nm, hb, HD), BF16),
            pltpu.VMEM((2, 2, nm, nm, hb, HD), BF16),
            pltpu.VMEM((2, 2, nm, nm, hb, HD), BF16),
            pltpu.VMEM((2, 2, nm, nm, hb, HD), BF16),
            pltpu.VMEM((2, 2, nm, hb, HD), BF16),
            pltpu.VMEM((2, 2, nm, hb, HD), BF16),
            pltpu.VMEM((2, nz, sub, HD), BF16),
            pltpu.VMEM((2, nz, sub, HD), BF16),
            dma((6,)),
            dma((1,)), dma((2, 5)),
            dma((2,)), dma((2, 5)),
            dma((2,)), dma((2, 5)),
            dma((2,)), dma((2, 5)),
            dma((1,)), dma((2, 2, nm)),
            dma((1,)), dma((2, 2)),
            dma((1,)), dma((2, 2)),
            dma((1,)), dma((2,)),
        ],
        compiler_params=pltpu.CompilerParams(
            collective_id=0, has_side_effects=True
        ),
    )(
        fork_pages, fork_visible,
        key_store.reshape(BLK, HD), value_store.reshape(BLK, HD),
        queries.reshape(rows, HD), upstream.reshape(rows, HD),
    )
    att, qg, kg, vg = pl.pallas_call(
        emit,
        out_shape=outs,
        in_specs=[vmem] * 4,
        out_specs=(hbm,) * 4,
        scratch_shapes=[dma((4,))],
        compiler_params=pltpu.CompilerParams(vmem_limit_bytes=4 * 2**20),
    )(*results)
    return (
        att.reshape(queries.shape), qg.reshape(queries.shape),
        kg.reshape(key_store.shape), vg.reshape(value_store.shape),
    )


def solution(mesh):
    nc = mesh.shape["seq"] // 2
    nx = 1
    while nx * nx < nc:
        nx *= 2
    placed = (
        P("seq", "head", None),
        P(("seq", "head"), None, None),
        P(("seq", "head"), None, None),
        P("seq", "head", None),
        P("seq", None),
        P("seq", None),
    )
    return jax.shard_map(
        functools.partial(per_device, nx, nc // nx, mesh.shape["head"]),
        mesh=mesh,
        in_specs=placed,
        out_specs=(
            P("seq", "head", None),
            P("seq", "head", None),
            P(("seq", "head"), None, None),
            P(("seq", "head"), None, None),
        ),
        check_vma=False,
    )
```

```python
import functools
import math

import jax
import jax.numpy as jnp
from jax import lax
from jax.experimental import pallas as pl
from jax.experimental.pallas import tpu as pltpu
from jax.sharding import PartitionSpec as P

HD = 128
BLK = 128
FORKS = 8
ENT = FORKS + 1
CW = 256
F32 = jnp.float32
BF16 = jnp.bfloat16
MESH = pl.DeviceIdType.MESH
NT = (((1,), (1,)), ((), ()))
FACTOR = 1.0 / math.sqrt(HD)
LOG2E = 1.4426950408889634
NEG = -1e30


def dot(a, b):
    return jnp.dot(a, b, preferred_element_type=F32)


def dot_nt(a, b):
    return lax.dot_general(a, b, NT, preferred_element_type=F32)


def remote(src, dst, send_sem, recv_sem, seq, head):
    return pltpu.make_async_remote_copy(
        src_ref=src, dst_ref=dst, send_sem=send_sem, recv_sem=recv_sem,
        device_id=(seq, head), device_id_type=MESH,
    )


def kernel(
    nx, ny, nz, groups,
    fork_hbm, vis_hbm, k_hbm, v_hbm, q_hbm, g_hbm,
    att_ref, qg_ref, kg_ref, vg_ref,
    kv_in, q_buf, g_buf, gt_buf, delta_buf, top_buf, sum_buf,
    zsrc, knear, kfar, vnear, vfar, ksel, vsel, kt_sel, vt_sel, s_buf, ds_buf,
    acc, fork_ref, vis_ref, slot_of, dsend, prec, rsend, rrec, ssend, srec, fin, zrec,
    io_sem, z_send, z_recv, la_send, la_recv, pa_send, pa_recv, fw_send, fw_recv,
    dd_send, dd_recv, r1_send, r1_recv, r2_send, r2_recv, zb_send, zb_recv,
):
    nc = nx * ny
    rows = BLK * groups
    chunks = rows // CW
    sub = BLK // nz
    hb = BLK // 2
    hz = nz // 2
    seq = lax.axis_index("seq")
    z = lax.axis_index("head")
    core = lax.rem(seq, 2)
    chip = seq // 2
    x = lax.rem(chip, nx)
    y = chip // nx
    partner = chip * 2 + (1 - core)

    def ring(d, n):
        return min(d, n - d)

    def far_first(n):
        return sorted(range(1, n), key=lambda d: -ring(d, n))

    rel = [(j + 1) // 2 if j % 2 else (nz - j // 2) % nz for j in range(nz)]
    slot_at = {r: j for j, r in enumerate(rel)}
    bounds = [0, 1, 4, 8] if nz == 8 else [0, 1, nz]
    parts = list(zip(bounds[:-1], bounds[1:]))
    part_of = [p for p, (lo, hi) in enumerate(parts) for _ in range(lo, hi)]

    def chip_at(dx, dy):
        return lax.rem(y + dy, ny) * nx + lax.rem(x + dx, nx)

    loads = [
        pltpu.make_async_copy(k_hbm, kv_in.at[0], io_sem.at[0]),
        pltpu.make_async_copy(v_hbm, kv_in.at[1], io_sem.at[1]),
        pltpu.make_async_copy(g_hbm, g_buf, io_sem.at[2]),
        pltpu.make_async_copy(q_hbm, q_buf, io_sem.at[3]),
        pltpu.make_async_copy(fork_hbm, fork_ref, io_sem.at[4]),
        pltpu.make_async_copy(vis_hbm, vis_ref, io_sem.at[5]),
    ]
    barrier = pltpu.get_barrier_semaphore()
    for o in range(1, nz):
        pl.semaphore_signal(barrier, inc=1, device_id=(seq, lax.rem(z + o, nz)), device_id_type=MESH)
    for d in far_first(nx):
        pl.semaphore_signal(barrier, inc=1, device_id=(chip_at(d, 0) * 2 + core, z), device_id_type=MESH)
    for d in far_first(ny):
        pl.semaphore_signal(barrier, inc=1, device_id=(chip_at(0, d) * 2 + core, z), device_id_type=MESH)
    pl.semaphore_signal(barrier, inc=1, device_id=(partner, z), device_id_type=MESH)
    for load in loads:
        load.start()

    r0 = lax.broadcasted_iota(jnp.int32, (BLK, BLK), 0)
    r1 = lax.broadcasted_iota(jnp.int32, (BLK, BLK), 1)

    def slot_head(j):
        return lax.rem(z + jnp.where(lax.rem(j, 2) == 1, (j + 1) // 2, nz - j // 2), nz)

    to_heads = (r1 == lax.rem(r0, sub) * nz + r0 // sub).astype(BF16)
    from_slots = (lax.rem(r0, nz) == slot_head(r1 // sub)) & (r0 // nz == lax.rem(r1, sub))
    from_slots = from_slots.astype(F32).astype(BF16)
    pages = ((knear, kfar), (vnear, vfar))
    for t in range(2):
        loads[t].wait()
        zsrc[t] = dot(to_heads, kv_in[t]).astype(BF16).reshape(nz, sub, HD)
        pages[t][0][y, x, core, 0] = zsrc[t, z]

    pl.semaphore_wait(barrier, nz - 1 + nx - 1 + ny - 1 + 1)

    def z_copy(t, o):
        head = lax.rem(z + o, nz)
        j = slot_at[(nz - o) % nz]
        dst = pages[t][j // hz].at[y, x, core, j % hz]
        return remote(zsrc.at[t, head], dst, z_send.at[0], z_recv.at[t, part_of[j]], seq, head)

    def x_first(t, k):
        return (t + k) % 2 == 0

    def spot(t, k, a, b):
        return chip_at(a, b) if x_first(t, k) else chip_at(b, a)

    def size_a(t, k):
        return nx if x_first(t, k) else ny

    def size_b(t, k):
        return ny if x_first(t, k) else nx

    def part_of_pages(t, part, ys, xs, cs):
        lo, hi = parts[part]
        return pages[t][lo // hz].at[ys, xs, cs, pl.ds(lo % hz, hi - lo)]

    def own_part(t, part):
        return part_of_pages(t, part, y, x, core)

    def line_send(t, part, d):
        ref = own_part(t, part)
        return remote(ref, ref, la_send.at[t], la_recv.at[t, part], spot(t, part, d, 0) * 2 + core, z)

    def line_arrivals(t, part):
        ref = part_of_pages(t, part, 0, pl.ds(0, size_a(t, part) - 1), 0)
        return remote(ref, ref, la_send.at[t], la_recv.at[t, part], partner, z)

    def plane_send(t, part, d):
        if x_first(t, part):
            ref = part_of_pages(t, part, y, pl.ds(0, nx), core)
        else:
            ref = part_of_pages(t, part, pl.ds(0, ny), x, core)
        return remote(ref, ref, pa_send.at[t], pa_recv.at[t, part], spot(t, part, 0, d) * 2 + core, z)

    def plane_arrivals(t, part):
        ref = part_of_pages(t, part, pl.ds(0, ny - 1), pl.ds(0, nx), 0)
        return remote(ref, ref, pa_send.at[t], pa_recv.at[t, part], partner, z)

    def page_forward(t, part):
        ref = part_of_pages(t, part, pl.ds(0, ny), pl.ds(0, nx), core)
        return remote(ref, ref, fw_send.at[t], fw_recv.at[t, part], partner, z)

    z_order = sorted(range(1, nz), key=lambda o: -ring(o, nz))
    for o in z_order:
        for t in range(2):
            z_copy(t, o).start()

    def send_part(part):
        for t in range(2):
            lo, hi = parts[part]
            first = max(lo, 1)
            if first < hi:
                here = pages[t][lo // hz].at[y, x, core, pl.ds(first % hz, hi - first)]
                remote(here, here, z_send.at[0], z_recv.at[t, part], seq, lax.rem(z + 1, nz)).wait_recv()
            for d in far_first(size_a(t, part)):
                line_send(t, part, d).start()

    def relay(part):
        for t in range(2):
            line_arrivals(t, part).wait_recv()
            for d in far_first(size_b(t, part)):
                plane_send(t, part, d).start()

    send_part(0)

    def entry_slots(p, _):
        first = jnp.int32(ENT)
        second = jnp.int32(ENT)
        for e in range(FORKS):
            hit = fork_ref[0, e] == p
            second = jnp.where(hit & (first < ENT), e + 1, second)
            first = jnp.where(hit & (first == ENT), e + 1, first)
        slot_of[0, p] = first
        slot_of[1, p] = second
        return 0

    loads[2].wait()
    for c in range(chunks):
        gt_buf[c] = g_buf[c * CW:(c + 1) * CW, :].T

    for part in range(1, len(parts)):
        send_part(part)
        if part > 1:
            relay(part - 2)
    for part in range(max(0, len(parts) - 2), len(parts)):
        relay(part)
    loads[4].wait()
    lax.fori_loop(0, 2 * nc, entry_slots, 0)
    for t in range(2):
        for h in range(2):
            acc[t, h] = jnp.zeros((ENT + 1, hb, HD), F32)

    def collect(t, part):
        plane_arrivals(t, part).wait_recv()
        page_forward(t, part).start()

    def collected(t, which):
        for part in which:
            page_forward(t, part).wait_recv()

    def page_at(p):
        return p // (2 * nx), lax.rem(p // 2, nx), lax.rem(p, 2)

    def select_pages(t, sel, h):
        for e in range(ENT):
            at = (y, x, core) if e == 0 else page_at(fork_ref[0, e - 1])
            page = pages[t][h][at[0], at[1], at[2]]
            sel[h, e * hb:(e + 1) * hb, :] = page.reshape(hb, HD)

    def transposed(sel, sel_t, h):
        for e in range(ENT):
            sel_t[h, :, e * hb:(e + 1) * hb] = sel[h, e * hb:(e + 1) * hb, :].T

    slot_row = lax.broadcasted_iota(jnp.int32, (hb, CW), 0)
    col = lax.broadcasted_iota(jnp.int32, (hb, CW), 1)

    def eights(a):
        return a.reshape(hb // 8, 8, CW)

    def lanes(c):
        return pl.ds(pl.multiple_of(c * CW, CW), CW)

    def scores(h):
        key_row = slot_head(h * hz + slot_row // sub) * sub + lax.rem(slot_row, sub)

        def step(c, _):
            q_c = q_buf[lanes(c), :]
            top = jnp.full((8, CW), NEG, F32)
            for e in range(ENT):
                raw = dot_nt(ksel[h, e * hb:(e + 1) * hb, :], q_c) * (FACTOR * LOG2E)
                if e == 0:
                    seen = key_row <= (col + c * CW) // groups
                else:
                    seen = key_row < vis_ref[0, e - 1]
                raw = jnp.where(seen, raw, NEG)
                s_buf[c, h, e] = raw
                top = jnp.maximum(top, jnp.max(eights(raw), axis=0))
            top = jnp.broadcast_to(jnp.max(top, axis=0, keepdims=True), (8, CW))
            total = jnp.zeros((8, CW), F32)
            for e in range(ENT):
                expo = jnp.exp2(s_buf[c, h, e] - top[:1])
                s_buf[c, h, e] = expo
                total = total + jnp.sum(eights(expo), axis=0)
            top_buf[c, h] = top
            sum_buf[c, h] = jnp.broadcast_to(jnp.sum(total, axis=0, keepdims=True), (8, CW))
            return 0

        lax.fori_loop(0, chunks, step, 0)

    near = range(part_of[hz])
    rest = range(part_of[hz], len(parts))
    for part in near:
        collect(0, part)
        collect(1, part)
    collected(0, near)
    select_pages(0, ksel, 0)
    loads[3].wait()
    loads[5].wait()
    scores(0)
    collected(1, near)
    select_pages(1, vsel, 0)
    transposed(vsel, vt_sel, 0)
    transposed(ksel, kt_sel, 0)
    for part in rest:
        collect(0, part)
        collect(1, part)
    collected(0, rest)
    select_pages(0, ksel, 1)
    scores(1)
    collected(1, rest)
    select_pages(1, vsel, 1)
    transposed(vsel, vt_sel, 1)

    def values(c, _):
        g_c = g_buf[lanes(c), :]
        top = jnp.maximum(top_buf[c, 0], top_buf[c, 1])
        scale = [jnp.exp2(top_buf[c, h] - top) for h in range(2)]
        inverse = 1.0 / (sum_buf[c, 0] * scale[0] + sum_buf[c, 1] * scale[1])
        out_t = jnp.zeros((HD, CW), F32)
        for h in range(2):
            factor = (scale[h] * inverse)[:1]
            for e in range(ENT):
                w = s_buf[c, h, e] * factor
                s_buf[c, h, e] = w
                ds_buf[c, h, e * hb:(e + 1) * hb, :] = w.astype(BF16)
            w_b = ds_buf[c, h]
            acc[1, h, :ENT] += dot(w_b, g_c).reshape(ENT, hb, HD)
            out_t = out_t + dot(vt_sel[h], w_b)
        out_b = out_t.astype(BF16)
        att_ref[lanes(c), :] = out_b.T
        delta = jnp.sum(out_b.astype(F32) * gt_buf[c].astype(F32), axis=0, keepdims=True)
        delta_buf[c] = jnp.broadcast_to(delta, (8, CW))
        return 0

    lax.fori_loop(0, chunks, values, 0)

    def slot_sum(t, h, page):
        return acc[t, h, slot_of[0, page]] + acc[t, h, slot_of[1, page]]

    def partner_send(t, h, a):
        return remote(dsend.at[t, h, a], prec.at[t, h, a], dd_send.at[0], dd_recv.at[t, h, a], partner, z)

    def first_send(t, h, a):
        to = spot(t, h, a, 0) * 2 + core
        return remote(rsend.at[t, h, a], rrec.at[t, h, a], r1_send.at[0], r1_recv.at[t, h], to, z)

    def second_send(t, h, b):
        to = spot(t, h, 0, b) * 2 + core
        return remote(ssend.at[t, h, b], srec.at[t, h, b], r2_send.at[0], r2_recv.at[t, h], to, z)

    def to_partner(t, h):
        for a in far_first(size_a(t, h)) + [0]:
            for b in range(size_b(t, h)):
                dsend[t, h, a, b] = slot_sum(t, h, spot(t, h, a, b) * 2 + (1 - core)).astype(BF16)
            partner_send(t, h, a).start()

    def mine(t, h, a, b):
        return slot_sum(t, h, spot(t, h, a, b) * 2 + core) + prec[t, h, a, b].astype(F32)

    def first_step(t, h, lo=0, hi=None):
        for a in far_first(size_a(t, h))[lo:hi]:
            partner_send(t, h, a).wait_recv()
            for b in range(size_b(t, h)):
                rsend[t, h, a, b] = mine(t, h, a, b).astype(BF16)
            first_send(t, h, a).start()

    def gathered(t, h, b):
        total = mine(t, h, 0, b)
        for a in range(1, size_a(t, h)):
            total = total + rrec[t, h, a, b].astype(F32)
        return total

    def second_step(t, h):
        partner_send(t, h, 0).wait_recv()
        here = rrec.at[t, h, pl.ds(1, size_a(t, h) - 1)]
        remote(here, here, r1_send.at[0], r1_recv.at[t, h], partner, z).wait_recv()
        for b in far_first(size_b(t, h)):
            ssend[t, h, b] = gathered(t, h, b).astype(BF16)
            second_send(t, h, b).start()

    def zb_copy(t, j):
        back = slot_at[(nz - rel[j]) % nz]
        return remote(fin.at[t, j], zrec.at[t, back], zb_send.at[0], zb_recv.at[t], seq, lax.rem(z + rel[j], nz))

    def finish(t, h):
        total = acc[t, h, 0] + gathered(t, h, 0)
        here = srec.at[t, h, pl.ds(1, size_b(t, h) - 1)]
        remote(here, here, r2_send.at[0], r2_recv.at[t, h], partner, z).wait_recv()
        for b in range(1, size_b(t, h)):
            total = total + srec[t, h, b].astype(F32)
        if t == 0:
            total = total * FACTOR
        fin[t, h * hz:(h + 1) * hz] = total.astype(BF16).reshape(hz, sub, HD)
        for j in range((h + 1) * hz - 1, h * hz - 1, -1):
            if j == 0:
                zrec[t, 0] = fin[t, 0]
            else:
                zb_copy(t, j).start()

    def result(t, out_ref):
        here = zrec.at[t, pl.ds(1, nz - 1)]
        remote(here, here, zb_send.at[0], zb_recv.at[t], seq, lax.rem(z + 1, nz)).wait_recv()
        out_ref[...] = dot(from_slots, zrec[t].reshape(BLK, HD)).astype(BF16)

    def grads(h):
        def step(c, _):
            g_c = g_buf[lanes(c), :]
            delta = delta_buf[c][:1]
            for e in range(ENT):
                part = pl.ds(e * hb, hb)
                ds_buf[c, h, part] = (s_buf[c, h, e] * (dot_nt(vsel[h, part], g_c) - delta)).astype(BF16)
            acc[0, h, :ENT] += dot(ds_buf[c, h], q_buf[lanes(c), :]).reshape(ENT, hb, HD)
            return 0

        lax.fori_loop(0, chunks, step, 0)

    def query_grads(c, _):
        dq_t = dot(kt_sel[0], ds_buf[c, 0]) + dot(kt_sel[1], ds_buf[c, 1])
        qg_ref[lanes(c), :] = (dq_t * FACTOR).T.astype(BF16)
        return 0

    to_partner(1, 1)
    to_partner(1, 0)
    grads(1)
    to_partner(0, 1)
    first_step(1, 1)
    first_step(1, 0, 0, 1)
    grads(0)
    to_partner(0, 0)
    first_step(0, 1)
    first_step(1, 0, 1)
    transposed(ksel, kt_sel, 1)
    first_step(0, 0)
    lax.fori_loop(0, chunks, query_grads, 0)
    second_step(1, 1)
    second_step(0, 1)
    second_step(1, 0)
    second_step(0, 0)
    finish(1, 1)
    finish(0, 1)
    finish(1, 0)
    finish(0, 0)
    result(1, vg_ref)
    result(0, kg_ref)


    def sent(ref, sem):
        remote(ref, ref, sem, r2_recv.at[0, 0], partner, z).wait_send()

    sent(zsrc.at[:, pl.ds(1, nz - 1)], z_send.at[0])
    sent(dsend, dd_send.at[0])
    sent(rsend.at[:, :, pl.ds(1, nx - 1)], r1_send.at[0])
    sent(ssend.at[:, :, pl.ds(1, nx - 1)], r2_send.at[0])
    sent(fin.at[:, pl.ds(1, nz - 1)], zb_send.at[0])
    for t in range(2):
        sent(pages[t][0].at[pl.ds(0, nx - 1), pl.ds(0, 2), 0], la_send.at[t])
        sent(pages[t][0].at[pl.ds(0, ny - 1)], pa_send.at[t])
        sent(pages[t][0], fw_send.at[t])


def emit(*refs):
    n = (len(refs) - 1) // 2
    copies = [pltpu.make_async_copy(refs[i], refs[n + i], refs[-1].at[i]) for i in range(n)]
    for copy in copies:
        copy.start()
    for copy in copies:
        copy.wait()


def per_device(nx, ny, nz, queries, key_store, value_store, upstream, fork_pages, fork_visible):
    groups = queries.shape[1]
    rows = BLK * groups
    chunks = rows // CW
    nc = nx * ny
    sub = BLK // nz
    hb = BLK // 2
    nm = max(nx, ny)
    dma = pltpu.SemaphoreType.DMA
    vmem = pl.BlockSpec(memory_space=pltpu.VMEM)
    hbm = pl.BlockSpec(memory_space=pltpu.HBM)
    big = jax.ShapeDtypeStruct((rows, HD), BF16)
    small = jax.ShapeDtypeStruct((BLK, HD), BF16)
    outs = (big, big, small, small)
    results = pl.pallas_call(
        functools.partial(kernel, nx, ny, nz, groups),
        out_shape=tuple(pltpu.VMEM(o.shape, BF16) for o in outs),
        in_specs=[hbm] * 6,
        out_specs=(vmem,) * 4,
        scratch_shapes=[
            pltpu.VMEM((2, BLK, HD), BF16),
            pltpu.VMEM((rows, HD), BF16),
            pltpu.VMEM((rows, HD), BF16),
            pltpu.VMEM((chunks, HD, CW), BF16),
            pltpu.VMEM((chunks, 8, CW), F32),
            pltpu.VMEM((chunks, 2, 8, CW), F32),
            pltpu.VMEM((chunks, 2, 8, CW), F32),
            pltpu.VMEM((2, nz, sub, HD), BF16),
            pltpu.VMEM((ny, nx, 2, nz // 2, sub, HD), BF16),
            pltpu.VMEM((ny, nx, 2, nz // 2, sub, HD), BF16),
            pltpu.VMEM((ny, nx, 2, nz // 2, sub, HD), BF16),
            pltpu.VMEM((ny, nx, 2, nz // 2, sub, HD), BF16),
            pltpu.VMEM((2, ENT * hb, HD), BF16),
            pltpu.VMEM((2, ENT * hb, HD), BF16),
            pltpu.VMEM((2, HD, ENT * hb), BF16),
            pltpu.VMEM((2, HD, ENT * hb), BF16),
            pltpu.VMEM((chunks, 2, ENT, hb, CW), F32),
            pltpu.VMEM((chunks, 2, ENT * hb, CW), BF16),
            pltpu.VMEM((2, 2, ENT + 1, hb, HD), F32),
            pltpu.SMEM((1, FORKS), jnp.int32),
            pltpu.SMEM((1, FORKS), jnp.int32),
            pltpu.SMEM((2, 2 * nc), jnp.int32),
            pltpu.VMEM((2, 2, nm, nm, hb, HD), BF16),
            pltpu.VMEM((2, 2, nm, nm, hb, HD), BF16),
            pltpu.VMEM((2, 2, nm, nm, hb, HD), BF16),
            pltpu.VMEM((2, 2, nm, nm, hb, HD), BF16),
            pltpu.VMEM((2, 2, nm, hb, HD), BF16),
            pltpu.VMEM((2, 2, nm, hb, HD), BF16),
            pltpu.VMEM((2, nz, sub, HD), BF16),
            pltpu.VMEM((2, nz, sub, HD), BF16),
            dma((6,)),
            dma((1,)), dma((2, 5)),
            dma((2,)), dma((2, 5)),
            dma((2,)), dma((2, 5)),
            dma((2,)), dma((2, 5)),
            dma((1,)), dma((2, 2, nm)),
            dma((1,)), dma((2, 2)),
            dma((1,)), dma((2, 2)),
            dma((1,)), dma((2,)),
        ],
        compiler_params=pltpu.CompilerParams(
            collective_id=0, has_side_effects=True
        ),
    )(
        fork_pages, fork_visible,
        key_store.reshape(BLK, HD), value_store.reshape(BLK, HD),
        queries.reshape(rows, HD), upstream.reshape(rows, HD),
    )
    att, qg, kg, vg = pl.pallas_call(
        emit,
        out_shape=outs,
        in_specs=[vmem] * 4,
        out_specs=(hbm,) * 4,
        scratch_shapes=[dma((4,))],
        compiler_params=pltpu.CompilerParams(vmem_limit_bytes=4 * 2**20),
    )(*results)
    return (
        att.reshape(queries.shape), qg.reshape(queries.shape),
        kg.reshape(key_store.shape), vg.reshape(value_store.shape),
    )


def solution(mesh):
    nc = mesh.shape["seq"] // 2
    nx = 1
    while nx * nx < nc:
        nx *= 2
    placed = (
        P("seq", "head", None),
        P(("seq", "head"), None, None),
        P(("seq", "head"), None, None),
        P("seq", "head", None),
        P("seq", None),
        P("seq", None),
    )
    return jax.shard_map(
        functools.partial(per_device, nx, nc // nx, mesh.shape["head"]),
        mesh=mesh,
        in_specs=placed,
        out_specs=(
            P("seq", "head", None),
            P("seq", "head", None),
            P(("seq", "head"), None, None),
            P(("seq", "head"), None, None),
        ),
        check_vma=False,
    )
```

```python
import functools
import math

import jax
import jax.numpy as jnp
from jax import lax
from jax.experimental import pallas as pl
from jax.experimental.pallas import tpu as pltpu
from jax.sharding import PartitionSpec as P

HD = 128
BLK = 128
FORKS = 8
ENT = FORKS + 1
CW = 256
F32 = jnp.float32
BF16 = jnp.bfloat16
MESH = pl.DeviceIdType.MESH
NT = (((1,), (1,)), ((), ()))
FACTOR = 1.0 / math.sqrt(HD)
LOG2E = 1.4426950408889634
NEG = -1e30


def dot(a, b):
    return jnp.dot(a, b, preferred_element_type=F32)


def dot_nt(a, b):
    return lax.dot_general(a, b, NT, preferred_element_type=F32)


def remote(src, dst, send_sem, recv_sem, seq, head):
    return pltpu.make_async_remote_copy(
        src_ref=src, dst_ref=dst, send_sem=send_sem, recv_sem=recv_sem,
        device_id=(seq, head), device_id_type=MESH,
    )


def kernel(
    nx, ny, nz, groups,
    fork_hbm, vis_hbm, k_hbm, v_hbm, q_hbm, g_hbm,
    att_ref, qg_ref, kg_ref, vg_ref,
    kv_in, q_buf, g_buf, gt_buf, delta_buf, top_buf, sum_buf,
    zsrc, knear, kfar, vnear, vfar, ksel, vsel, kt_sel, vt_sel, s_buf, ds_buf,
    acc, fork_ref, vis_ref, slot_of, dsend, prec, rsend, rrec, ssend, srec, fin, zrec,
    io_sem, z_send, z_recv, la_send, la_recv, pa_send, pa_recv, fw_send, fw_recv,
    dd_send, dd_recv, r1_send, r1_recv, r2_send, r2_recv, zb_send, zb_recv,
):
    nc = nx * ny
    rows = BLK * groups
    chunks = rows // CW
    sub = BLK // nz
    hb = BLK // 2
    hz = nz // 2
    seq = lax.axis_index("seq")
    z = lax.axis_index("head")
    core = lax.rem(seq, 2)
    chip = seq // 2
    x = lax.rem(chip, nx)
    y = chip // nx
    partner = chip * 2 + (1 - core)

    def ring(d, n):
        return min(d, n - d)

    def far_first(n):
        return sorted(range(1, n), key=lambda d: -ring(d, n))

    rel = [(j + 1) // 2 if j % 2 else (nz - j // 2) % nz for j in range(nz)]
    slot_at = {r: j for j, r in enumerate(rel)}
    bounds = [0, 1, 4, 8] if nz == 8 else [0, 1, nz]
    parts = list(zip(bounds[:-1], bounds[1:]))
    part_of = [p for p, (lo, hi) in enumerate(parts) for _ in range(lo, hi)]

    def chip_at(dx, dy):
        return lax.rem(y + dy, ny) * nx + lax.rem(x + dx, nx)

    loads = [
        pltpu.make_async_copy(k_hbm, kv_in.at[0], io_sem.at[0]),
        pltpu.make_async_copy(v_hbm, kv_in.at[1], io_sem.at[1]),
        pltpu.make_async_copy(g_hbm, g_buf, io_sem.at[2]),
        pltpu.make_async_copy(q_hbm, q_buf, io_sem.at[3]),
        pltpu.make_async_copy(fork_hbm, fork_ref, io_sem.at[4]),
        pltpu.make_async_copy(vis_hbm, vis_ref, io_sem.at[5]),
    ]
    barrier = pltpu.get_barrier_semaphore()
    for o in range(1, nz):
        pl.semaphore_signal(barrier, inc=1, device_id=(seq, lax.rem(z + o, nz)), device_id_type=MESH)
    for d in far_first(nx):
        pl.semaphore_signal(barrier, inc=1, device_id=(chip_at(d, 0) * 2 + core, z), device_id_type=MESH)
    for d in far_first(ny):
        pl.semaphore_signal(barrier, inc=1, device_id=(chip_at(0, d) * 2 + core, z), device_id_type=MESH)
    pl.semaphore_signal(barrier, inc=1, device_id=(partner, z), device_id_type=MESH)
    for load in loads:
        load.start()

    r0 = lax.broadcasted_iota(jnp.int32, (BLK, BLK), 0)
    r1 = lax.broadcasted_iota(jnp.int32, (BLK, BLK), 1)

    def slot_head(j):
        return lax.rem(z + jnp.where(lax.rem(j, 2) == 1, (j + 1) // 2, nz - j // 2), nz)

    to_heads = (r1 == lax.rem(r0, sub) * nz + r0 // sub).astype(BF16)
    from_slots = (lax.rem(r0, nz) == slot_head(r1 // sub)) & (r0 // nz == lax.rem(r1, sub))
    from_slots = from_slots.astype(F32).astype(BF16)
    pages = ((knear, kfar), (vnear, vfar))
    for t in range(2):
        loads[t].wait()
        zsrc[t] = dot(to_heads, kv_in[t]).astype(BF16).reshape(nz, sub, HD)
        pages[t][0][y, x, core, 0] = zsrc[t, z]

    pl.semaphore_wait(barrier, nz - 1 + nx - 1 + ny - 1 + 1)

    def z_copy(t, o):
        head = lax.rem(z + o, nz)
        j = slot_at[(nz - o) % nz]
        dst = pages[t][j // hz].at[y, x, core, j % hz]
        return remote(zsrc.at[t, head], dst, z_send.at[0], z_recv.at[t, part_of[j]], seq, head)

    def x_first(t, k):
        return (t + k) % 2 == 0

    def spot(t, k, a, b):
        return chip_at(a, b) if x_first(t, k) else chip_at(b, a)

    def size_a(t, k):
        return nx if x_first(t, k) else ny

    def size_b(t, k):
        return ny if x_first(t, k) else nx

    def part_of_pages(t, part, ys, xs, cs):
        lo, hi = parts[part]
        return pages[t][lo // hz].at[ys, xs, cs, pl.ds(lo % hz, hi - lo)]

    def own_part(t, part):
        return part_of_pages(t, part, y, x, core)

    def line_send(t, part, d):
        ref = own_part(t, part)
        return remote(ref, ref, la_send.at[t], la_recv.at[t, part], spot(t, part, d, 0) * 2 + core, z)

    def line_arrivals(t, part):
        ref = part_of_pages(t, part, 0, pl.ds(0, size_a(t, part) - 1), 0)
        return remote(ref, ref, la_send.at[t], la_recv.at[t, part], partner, z)

    def plane_send(t, part, d):
        if x_first(t, part):
            ref = part_of_pages(t, part, y, pl.ds(0, nx), core)
        else:
            ref = part_of_pages(t, part, pl.ds(0, ny), x, core)
        return remote(ref, ref, pa_send.at[t], pa_recv.at[t, part], spot(t, part, 0, d) * 2 + core, z)

    def plane_arrivals(t, part):
        ref = part_of_pages(t, part, pl.ds(0, ny - 1), pl.ds(0, nx), 0)
        return remote(ref, ref, pa_send.at[t], pa_recv.at[t, part], partner, z)

    def page_forward(t, part):
        ref = part_of_pages(t, part, pl.ds(0, ny), pl.ds(0, nx), core)
        return remote(ref, ref, fw_send.at[t], fw_recv.at[t, part], partner, z)

    z_order = sorted(range(1, nz), key=lambda o: -ring(o, nz))
    for o in z_order:
        for t in range(2):
            z_copy(t, o).start()

    def send_part(part):
        for t in range(2):
            lo, hi = parts[part]
            first = max(lo, 1)
            if first < hi:
                here = pages[t][lo // hz].at[y, x, core, pl.ds(first % hz, hi - first)]
                remote(here, here, z_send.at[0], z_recv.at[t, part], seq, lax.rem(z + 1, nz)).wait_recv()
            for d in far_first(size_a(t, part)):
                line_send(t, part, d).start()

    def relay(part):
        for t in range(2):
            line_arrivals(t, part).wait_recv()
            for d in far_first(size_b(t, part)):
                plane_send(t, part, d).start()

    send_part(0)

    def entry_slots(p, _):
        first = jnp.int32(ENT)
        second = jnp.int32(ENT)
        for e in range(FORKS):
            hit = fork_ref[0, e] == p
            second = jnp.where(hit & (first < ENT), e + 1, second)
            first = jnp.where(hit & (first == ENT), e + 1, first)
        slot_of[0, p] = first
        slot_of[1, p] = second
        return 0

    loads[2].wait()
    for c in range(chunks):
        gt_buf[c] = g_buf[c * CW:(c + 1) * CW, :].T

    for part in range(1, len(parts)):
        send_part(part)
        if part > 1:
            relay(part - 2)
    for part in range(max(0, len(parts) - 2), len(parts)):
        relay(part)
    loads[4].wait()
    lax.fori_loop(0, 2 * nc, entry_slots, 0)
    for t in range(2):
        for h in range(2):
            acc[t, h] = jnp.zeros((ENT + 1, hb, HD), F32)

    def collect(t, part):
        plane_arrivals(t, part).wait_recv()
        page_forward(t, part).start()

    def collected(t, which):
        for part in which:
            page_forward(t, part).wait_recv()

    def page_at(p):
        return p // (2 * nx), lax.rem(p // 2, nx), lax.rem(p, 2)

    def select_pages(t, sel, h):
        for e in range(ENT):
            at = (y, x, core) if e == 0 else page_at(fork_ref[0, e - 1])
            page = pages[t][h][at[0], at[1], at[2]]
            sel[h, e * hb:(e + 1) * hb, :] = page.reshape(hb, HD)

    def transposed(sel, sel_t, h):
        for e in range(ENT):
            sel_t[h, :, e * hb:(e + 1) * hb] = sel[h, e * hb:(e + 1) * hb, :].T

    slot_row = lax.broadcasted_iota(jnp.int32, (hb, CW), 0)
    col = lax.broadcasted_iota(jnp.int32, (hb, CW), 1)

    def eights(a):
        return a.reshape(hb // 8, 8, CW)

    def lanes(c):
        return pl.ds(pl.multiple_of(c * CW, CW), CW)

    def scores(h):
        key_row = slot_head(h * hz + slot_row // sub) * sub + lax.rem(slot_row, sub)

        def step(c, _):
            q_c = q_buf[lanes(c), :]
            top = jnp.full((8, CW), NEG, F32)
            for e in range(ENT):
                raw = dot_nt(ksel[h, e * hb:(e + 1) * hb, :], q_c) * (FACTOR * LOG2E)
                if e == 0:
                    seen = key_row <= (col + c * CW) // groups
                else:
                    seen = key_row < vis_ref[0, e - 1]
                raw = jnp.where(seen, raw, NEG)
                s_buf[c, h, e] = raw
                top = jnp.maximum(top, jnp.max(eights(raw), axis=0))
            top = jnp.broadcast_to(jnp.max(top, axis=0, keepdims=True), (8, CW))
            total = jnp.zeros((8, CW), F32)
            for e in range(ENT):
                expo = jnp.exp2(s_buf[c, h, e] - top[:1])
                s_buf[c, h, e] = expo
                total = total + jnp.sum(eights(expo), axis=0)
            top_buf[c, h] = top
            sum_buf[c, h] = jnp.broadcast_to(jnp.sum(total, axis=0, keepdims=True), (8, CW))
            return 0

        lax.fori_loop(0, chunks, step, 0)

    near = range(part_of[hz])
    rest = range(part_of[hz], len(parts))
    for part in near:
        collect(0, part)
        collect(1, part)
    collected(0, near)
    select_pages(0, ksel, 0)
    loads[3].wait()
    loads[5].wait()
    scores(0)
    collected(1, near)
    select_pages(1, vsel, 0)
    transposed(vsel, vt_sel, 0)
    transposed(ksel, kt_sel, 0)
    for part in rest:
        collect(0, part)
        collect(1, part)
    collected(0, rest)
    select_pages(0, ksel, 1)
    scores(1)
    def weigh(c, _):
        g_c = g_buf[lanes(c), :]
        top = jnp.maximum(top_buf[c, 0], top_buf[c, 1])
        scale = [jnp.exp2(top_buf[c, h] - top) for h in range(2)]
        inverse = 1.0 / (sum_buf[c, 0] * scale[0] + sum_buf[c, 1] * scale[1])
        for h in range(2):
            factor = (scale[h] * inverse)[:1]
            for e in range(ENT):
                w = s_buf[c, h, e] * factor
                s_buf[c, h, e] = w
                ds_buf[c, h, e * hb:(e + 1) * hb, :] = w.astype(BF16)
            acc[1, h, :ENT] += dot(ds_buf[c, h], g_c).reshape(ENT, hb, HD)
        return 0

    def attend(c, _):
        out_b = (dot(vt_sel[0], ds_buf[c, 0]) + dot(vt_sel[1], ds_buf[c, 1])).astype(BF16)
        att_ref[lanes(c), :] = out_b.T
        delta = jnp.sum(out_b.astype(F32) * gt_buf[c].astype(F32), axis=0, keepdims=True)
        delta_buf[c] = jnp.broadcast_to(delta, (8, CW))
        return 0

    def slot_sum(t, h, page):
        return acc[t, h, slot_of[0, page]] + acc[t, h, slot_of[1, page]]

    def partner_send(t, h, a):
        return remote(dsend.at[t, h, a], prec.at[t, h, a], dd_send.at[0], dd_recv.at[t, h, a], partner, z)

    def first_send(t, h, a):
        to = spot(t, h, a, 0) * 2 + core
        return remote(rsend.at[t, h, a], rrec.at[t, h, a], r1_send.at[0], r1_recv.at[t, h], to, z)

    def second_send(t, h, b):
        to = spot(t, h, 0, b) * 2 + core
        return remote(ssend.at[t, h, b], srec.at[t, h, b], r2_send.at[0], r2_recv.at[t, h], to, z)

    def to_partner(t, h):
        for a in far_first(size_a(t, h)) + [0]:
            for b in range(size_b(t, h)):
                dsend[t, h, a, b] = slot_sum(t, h, spot(t, h, a, b) * 2 + (1 - core)).astype(BF16)
            partner_send(t, h, a).start()

    def mine(t, h, a, b):
        return slot_sum(t, h, spot(t, h, a, b) * 2 + core) + prec[t, h, a, b].astype(F32)

    def first_step(t, h, lo=0, hi=None):
        for a in far_first(size_a(t, h))[lo:hi]:
            partner_send(t, h, a).wait_recv()
            for b in range(size_b(t, h)):
                rsend[t, h, a, b] = mine(t, h, a, b).astype(BF16)
            first_send(t, h, a).start()

    def gathered(t, h, b):
        total = mine(t, h, 0, b)
        for a in range(1, size_a(t, h)):
            total = total + rrec[t, h, a, b].astype(F32)
        return total

    def second_step(t, h):
        partner_send(t, h, 0).wait_recv()
        here = rrec.at[t, h, pl.ds(1, size_a(t, h) - 1)]
        remote(here, here, r1_send.at[0], r1_recv.at[t, h], partner, z).wait_recv()
        for b in far_first(size_b(t, h)):
            ssend[t, h, b] = gathered(t, h, b).astype(BF16)
            second_send(t, h, b).start()

    def zb_copy(t, j):
        back = slot_at[(nz - rel[j]) % nz]
        return remote(fin.at[t, j], zrec.at[t, back], zb_send.at[0], zb_recv.at[t], seq, lax.rem(z + rel[j], nz))

    def finish(t, h):
        total = acc[t, h, 0] + gathered(t, h, 0)
        here = srec.at[t, h, pl.ds(1, size_b(t, h) - 1)]
        remote(here, here, r2_send.at[0], r2_recv.at[t, h], partner, z).wait_recv()
        for b in range(1, size_b(t, h)):
            total = total + srec[t, h, b].astype(F32)
        if t == 0:
            total = total * FACTOR
        fin[t, h * hz:(h + 1) * hz] = total.astype(BF16).reshape(hz, sub, HD)
        for j in range((h + 1) * hz - 1, h * hz - 1, -1):
            if j == 0:
                zrec[t, 0] = fin[t, 0]
            else:
                zb_copy(t, j).start()

    def result(t, out_ref):
        here = zrec.at[t, pl.ds(1, nz - 1)]
        remote(here, here, zb_send.at[0], zb_recv.at[t], seq, lax.rem(z + 1, nz)).wait_recv()
        out_ref[...] = dot(from_slots, zrec[t].reshape(BLK, HD)).astype(BF16)

    def grads(h):
        def step(c, _):
            g_c = g_buf[lanes(c), :]
            delta = delta_buf[c][:1]
            for e in range(ENT):
                part = pl.ds(e * hb, hb)
                ds_buf[c, h, part] = (s_buf[c, h, e] * (dot_nt(vsel[h, part], g_c) - delta)).astype(BF16)
            acc[0, h, :ENT] += dot(ds_buf[c, h], q_buf[lanes(c), :]).reshape(ENT, hb, HD)
            return 0

        lax.fori_loop(0, chunks, step, 0)

    def query_grads(c, _):
        dq_t = dot(kt_sel[0], ds_buf[c, 0]) + dot(kt_sel[1], ds_buf[c, 1])
        qg_ref[lanes(c), :] = (dq_t * FACTOR).T.astype(BF16)
        return 0

    lax.fori_loop(0, chunks, weigh, 0)
    to_partner(1, 1)
    to_partner(1, 0)
    collected(1, rest)
    select_pages(1, vsel, 1)
    transposed(vsel, vt_sel, 1)
    lax.fori_loop(0, chunks, attend, 0)
    first_step(1, 1)
    first_step(1, 0, 0, 1)
    grads(1)
    to_partner(0, 1)
    grads(0)
    to_partner(0, 0)
    first_step(0, 1)
    first_step(1, 0, 1)
    transposed(ksel, kt_sel, 1)
    first_step(0, 0)
    lax.fori_loop(0, chunks, query_grads, 0)
    second_step(1, 1)
    second_step(0, 1)
    second_step(1, 0)
    second_step(0, 0)
    finish(1, 1)
    finish(0, 1)
    finish(1, 0)
    finish(0, 0)
    result(1, vg_ref)
    result(0, kg_ref)


    def sent(ref, sem):
        remote(ref, ref, sem, r2_recv.at[0, 0], partner, z).wait_send()

    sent(zsrc.at[:, pl.ds(1, nz - 1)], z_send.at[0])
    sent(dsend, dd_send.at[0])
    sent(rsend.at[:, :, pl.ds(1, nx - 1)], r1_send.at[0])
    sent(ssend.at[:, :, pl.ds(1, nx - 1)], r2_send.at[0])
    sent(fin.at[:, pl.ds(1, nz - 1)], zb_send.at[0])
    for t in range(2):
        sent(pages[t][0].at[pl.ds(0, nx - 1), pl.ds(0, 2), 0], la_send.at[t])
        sent(pages[t][0].at[pl.ds(0, ny - 1)], pa_send.at[t])
        sent(pages[t][0], fw_send.at[t])


def emit(*refs):
    n = (len(refs) - 1) // 2
    copies = [pltpu.make_async_copy(refs[i], refs[n + i], refs[-1].at[i]) for i in range(n)]
    for copy in copies:
        copy.start()
    for copy in copies:
        copy.wait()


def per_device(nx, ny, nz, queries, key_store, value_store, upstream, fork_pages, fork_visible):
    groups = queries.shape[1]
    rows = BLK * groups
    chunks = rows // CW
    nc = nx * ny
    sub = BLK // nz
    hb = BLK // 2
    nm = max(nx, ny)
    dma = pltpu.SemaphoreType.DMA
    vmem = pl.BlockSpec(memory_space=pltpu.VMEM)
    hbm = pl.BlockSpec(memory_space=pltpu.HBM)
    big = jax.ShapeDtypeStruct((rows, HD), BF16)
    small = jax.ShapeDtypeStruct((BLK, HD), BF16)
    outs = (big, big, small, small)
    results = pl.pallas_call(
        functools.partial(kernel, nx, ny, nz, groups),
        out_shape=tuple(pltpu.VMEM(o.shape, BF16) for o in outs),
        in_specs=[hbm] * 6,
        out_specs=(vmem,) * 4,
        scratch_shapes=[
            pltpu.VMEM((2, BLK, HD), BF16),
            pltpu.VMEM((rows, HD), BF16),
            pltpu.VMEM((rows, HD), BF16),
            pltpu.VMEM((chunks, HD, CW), BF16),
            pltpu.VMEM((chunks, 8, CW), F32),
            pltpu.VMEM((chunks, 2, 8, CW), F32),
            pltpu.VMEM((chunks, 2, 8, CW), F32),
            pltpu.VMEM((2, nz, sub, HD), BF16),
            pltpu.VMEM((ny, nx, 2, nz // 2, sub, HD), BF16),
            pltpu.VMEM((ny, nx, 2, nz // 2, sub, HD), BF16),
            pltpu.VMEM((ny, nx, 2, nz // 2, sub, HD), BF16),
            pltpu.VMEM((ny, nx, 2, nz // 2, sub, HD), BF16),
            pltpu.VMEM((2, ENT * hb, HD), BF16),
            pltpu.VMEM((2, ENT * hb, HD), BF16),
            pltpu.VMEM((2, HD, ENT * hb), BF16),
            pltpu.VMEM((2, HD, ENT * hb), BF16),
            pltpu.VMEM((chunks, 2, ENT, hb, CW), F32),
            pltpu.VMEM((chunks, 2, ENT * hb, CW), BF16),
            pltpu.VMEM((2, 2, ENT + 1, hb, HD), F32),
            pltpu.SMEM((1, FORKS), jnp.int32),
            pltpu.SMEM((1, FORKS), jnp.int32),
            pltpu.SMEM((2, 2 * nc), jnp.int32),
            pltpu.VMEM((2, 2, nm, nm, hb, HD), BF16),
            pltpu.VMEM((2, 2, nm, nm, hb, HD), BF16),
            pltpu.VMEM((2, 2, nm, nm, hb, HD), BF16),
            pltpu.VMEM((2, 2, nm, nm, hb, HD), BF16),
            pltpu.VMEM((2, 2, nm, hb, HD), BF16),
            pltpu.VMEM((2, 2, nm, hb, HD), BF16),
            pltpu.VMEM((2, nz, sub, HD), BF16),
            pltpu.VMEM((2, nz, sub, HD), BF16),
            dma((6,)),
            dma((1,)), dma((2, 5)),
            dma((2,)), dma((2, 5)),
            dma((2,)), dma((2, 5)),
            dma((2,)), dma((2, 5)),
            dma((1,)), dma((2, 2, nm)),
            dma((1,)), dma((2, 2)),
            dma((1,)), dma((2, 2)),
            dma((1,)), dma((2,)),
        ],
        compiler_params=pltpu.CompilerParams(
            collective_id=0, has_side_effects=True
        ),
    )(
        fork_pages, fork_visible,
        key_store.reshape(BLK, HD), value_store.reshape(BLK, HD),
        queries.reshape(rows, HD), upstream.reshape(rows, HD),
    )
    att, qg, kg, vg = pl.pallas_call(
        emit,
        out_shape=outs,
        in_specs=[vmem] * 4,
        out_specs=(hbm,) * 4,
        scratch_shapes=[dma((4,))],
        compiler_params=pltpu.CompilerParams(vmem_limit_bytes=4 * 2**20),
    )(*results)
    return (
        att.reshape(queries.shape), qg.reshape(queries.shape),
        kg.reshape(key_store.shape), vg.reshape(value_store.shape),
    )


def solution(mesh):
    nc = mesh.shape["seq"] // 2
    nx = 1
    while nx * nx < nc:
        nx *= 2
    placed = (
        P("seq", "head", None),
        P(("seq", "head"), None, None),
        P(("seq", "head"), None, None),
        P("seq", "head", None),
        P("seq", None),
        P("seq", None),
    )
    return jax.shard_map(
        functools.partial(per_device, nx, nc // nx, mesh.shape["head"]),
        mesh=mesh,
        in_specs=placed,
        out_specs=(
            P("seq", "head", None),
            P("seq", "head", None),
            P(("seq", "head"), None, None),
            P(("seq", "head"), None, None),
        ),
        check_vma=False,
    )
```

```python
import functools
import math

import jax
import jax.numpy as jnp
from jax import lax
from jax.experimental import pallas as pl
from jax.experimental.pallas import tpu as pltpu
from jax.sharding import PartitionSpec as P

HD = 128
BLK = 128
FORKS = 8
ENT = FORKS + 1
CW = 256
F32 = jnp.float32
BF16 = jnp.bfloat16
MESH = pl.DeviceIdType.MESH
NT = (((1,), (1,)), ((), ()))
FACTOR = 1.0 / math.sqrt(HD)
LOG2E = 1.4426950408889634
NEG = -1e30


def dot(a, b):
    return jnp.dot(a, b, preferred_element_type=F32)


def dot_nt(a, b):
    return lax.dot_general(a, b, NT, preferred_element_type=F32)


def remote(src, dst, send_sem, recv_sem, seq, head):
    return pltpu.make_async_remote_copy(
        src_ref=src, dst_ref=dst, send_sem=send_sem, recv_sem=recv_sem,
        device_id=(seq, head), device_id_type=MESH,
    )


def kernel(
    nx, ny, nz, groups,
    fork_hbm, vis_hbm, k_hbm, v_hbm, q_hbm, g_hbm,
    att_ref, qg_ref, kg_ref, vg_ref,
    kv_in, q_buf, g_buf, gt_buf, delta_buf, top_buf, sum_buf,
    zsrc, knear, kfar, vnear, vfar, ksel, vsel, kt_sel, vt_sel, s_buf, ds_buf,
    acc, fork_ref, vis_ref, slot_of, dsend, prec, rsend, rrec, ssend, srec, fin, zrec,
    io_sem, z_send, z_recv, la_send, la_recv, pa_send, pa_recv, fw_send, fw_recv,
    dd_send, dd_recv, r1_send, r1_recv, r2_send, r2_recv, zb_send, zb_recv,
):
    nc = nx * ny
    rows = BLK * groups
    chunks = rows // CW
    sub = BLK // nz
    hb = BLK // 2
    hz = nz // 2
    seq = lax.axis_index("seq")
    z = lax.axis_index("head")
    core = lax.rem(seq, 2)
    chip = seq // 2
    x = lax.rem(chip, nx)
    y = chip // nx
    partner = chip * 2 + (1 - core)

    def ring(d, n):
        return min(d, n - d)

    def far_first(n):
        return sorted(range(1, n), key=lambda d: -ring(d, n))

    rel = [(j + 1) // 2 if j % 2 else (nz - j // 2) % nz for j in range(nz)]
    slot_at = {r: j for j, r in enumerate(rel)}
    bounds = [0, 1, 4, 8] if nz == 8 else [0, 1, nz]
    parts = list(zip(bounds[:-1], bounds[1:]))
    part_of = [p for p, (lo, hi) in enumerate(parts) for _ in range(lo, hi)]

    def chip_at(dx, dy):
        return lax.rem(y + dy, ny) * nx + lax.rem(x + dx, nx)

    loads = [
        pltpu.make_async_copy(k_hbm, kv_in.at[0], io_sem.at[0]),
        pltpu.make_async_copy(v_hbm, kv_in.at[1], io_sem.at[1]),
        pltpu.make_async_copy(g_hbm, g_buf, io_sem.at[2]),
        pltpu.make_async_copy(q_hbm, q_buf, io_sem.at[3]),
        pltpu.make_async_copy(fork_hbm, fork_ref, io_sem.at[4]),
        pltpu.make_async_copy(vis_hbm, vis_ref, io_sem.at[5]),
    ]
    barrier = pltpu.get_barrier_semaphore()
    for o in range(1, nz):
        pl.semaphore_signal(barrier, inc=1, device_id=(seq, lax.rem(z + o, nz)), device_id_type=MESH)
    for d in far_first(nx):
        pl.semaphore_signal(barrier, inc=1, device_id=(chip_at(d, 0) * 2 + core, z), device_id_type=MESH)
    for d in far_first(ny):
        pl.semaphore_signal(barrier, inc=1, device_id=(chip_at(0, d) * 2 + core, z), device_id_type=MESH)
    pl.semaphore_signal(barrier, inc=1, device_id=(partner, z), device_id_type=MESH)
    for load in loads:
        load.start()

    r0 = lax.broadcasted_iota(jnp.int32, (BLK, BLK), 0)
    r1 = lax.broadcasted_iota(jnp.int32, (BLK, BLK), 1)

    def slot_head(j):
        return lax.rem(z + jnp.where(lax.rem(j, 2) == 1, (j + 1) // 2, nz - j // 2), nz)

    to_heads = (r1 == lax.rem(r0, sub) * nz + r0 // sub).astype(BF16)
    from_slots = (lax.rem(r0, nz) == slot_head(r1 // sub)) & (r0 // nz == lax.rem(r1, sub))
    from_slots = from_slots.astype(F32).astype(BF16)
    pages = ((knear, kfar), (vnear, vfar))
    for t in range(2):
        loads[t].wait()
        zsrc[t] = dot(to_heads, kv_in[t]).astype(BF16).reshape(nz, sub, HD)
        pages[t][0][y, x, core, 0] = zsrc[t, z]

    pl.semaphore_wait(barrier, nz - 1 + nx - 1 + ny - 1 + 1)

    def z_copy(t, o):
        head = lax.rem(z + o, nz)
        j = slot_at[(nz - o) % nz]
        dst = pages[t][j // hz].at[y, x, core, j % hz]
        return remote(zsrc.at[t, head], dst, z_send.at[0], z_recv.at[t, part_of[j]], seq, head)

    def x_first(t, k):
        return (t + k) % 2 == 0

    def spot(t, k, a, b):
        return chip_at(a, b) if x_first(t, k) else chip_at(b, a)

    def size_a(t, k):
        return nx if x_first(t, k) else ny

    def size_b(t, k):
        return ny if x_first(t, k) else nx

    def part_of_pages(t, part, ys, xs, cs):
        lo, hi = parts[part]
        return pages[t][lo // hz].at[ys, xs, cs, pl.ds(lo % hz, hi - lo)]

    def own_part(t, part):
        return part_of_pages(t, part, y, x, core)

    def line_send(t, part, d):
        ref = own_part(t, part)
        return remote(ref, ref, la_send.at[t], la_recv.at[t, part], spot(t, part, d, 0) * 2 + core, z)

    def line_arrivals(t, part):
        ref = part_of_pages(t, part, 0, pl.ds(0, size_a(t, part) - 1), 0)
        return remote(ref, ref, la_send.at[t], la_recv.at[t, part], partner, z)

    def plane_send(t, part, d):
        if x_first(t, part):
            ref = part_of_pages(t, part, y, pl.ds(0, nx), core)
        else:
            ref = part_of_pages(t, part, pl.ds(0, ny), x, core)
        return remote(ref, ref, pa_send.at[t], pa_recv.at[t, part], spot(t, part, 0, d) * 2 + core, z)

    def plane_arrivals(t, part):
        ref = part_of_pages(t, part, pl.ds(0, ny - 1), pl.ds(0, nx), 0)
        return remote(ref, ref, pa_send.at[t], pa_recv.at[t, part], partner, z)

    def page_forward(t, part):
        ref = part_of_pages(t, part, pl.ds(0, ny), pl.ds(0, nx), core)
        return remote(ref, ref, fw_send.at[t], fw_recv.at[t, part], partner, z)

    z_order = sorted(range(1, nz), key=lambda o: -ring(o, nz))
    for o in z_order:
        for t in range(2):
            z_copy(t, o).start()

    def send_part(part):
        for t in range(2):
            lo, hi = parts[part]
            first = max(lo, 1)
            if first < hi:
                here = pages[t][lo // hz].at[y, x, core, pl.ds(first % hz, hi - first)]
                remote(here, here, z_send.at[0], z_recv.at[t, part], seq, lax.rem(z + 1, nz)).wait_recv()
            for d in far_first(size_a(t, part)):
                line_send(t, part, d).start()

    def relay(part):
        for t in range(2):
            line_arrivals(t, part).wait_recv()
            for d in far_first(size_b(t, part)):
                plane_send(t, part, d).start()

    send_part(0)

    def entry_slots(p, _):
        first = jnp.int32(ENT)
        second = jnp.int32(ENT)
        for e in range(FORKS):
            hit = fork_ref[0, e] == p
            second = jnp.where(hit & (first < ENT), e + 1, second)
            first = jnp.where(hit & (first == ENT), e + 1, first)
        slot_of[0, p] = first
        slot_of[1, p] = second
        return 0

    loads[2].wait()
    for c in range(chunks):
        gt_buf[c] = g_buf[c * CW:(c + 1) * CW, :].T

    for part in range(1, len(parts)):
        send_part(part)
        relay(part - 1)
    relay(len(parts) - 1)
    loads[4].wait()
    lax.fori_loop(0, 2 * nc, entry_slots, 0)
    for t in range(2):
        for h in range(2):
            acc[t, h] = jnp.zeros((ENT + 1, hb, HD), F32)

    def collect(t, part):
        plane_arrivals(t, part).wait_recv()
        page_forward(t, part).start()

    def collected(t, which):
        for part in which:
            page_forward(t, part).wait_recv()

    def page_at(p):
        return p // (2 * nx), lax.rem(p // 2, nx), lax.rem(p, 2)

    def select_pages(t, sel, h):
        for e in range(ENT):
            at = (y, x, core) if e == 0 else page_at(fork_ref[0, e - 1])
            page = pages[t][h][at[0], at[1], at[2]]
            sel[h, e * hb:(e + 1) * hb, :] = page.reshape(hb, HD)

    def transposed(sel, sel_t, h):
        for e in range(ENT):
            sel_t[h, :, e * hb:(e + 1) * hb] = sel[h, e * hb:(e + 1) * hb, :].T

    slot_row = lax.broadcasted_iota(jnp.int32, (hb, CW), 0)
    col = lax.broadcasted_iota(jnp.int32, (hb, CW), 1)

    def eights(a):
        return a.reshape(hb // 8, 8, CW)

    def lanes(c):
        return pl.ds(pl.multiple_of(c * CW, CW), CW)

    def scores(h):
        key_row = slot_head(h * hz + slot_row // sub) * sub + lax.rem(slot_row, sub)

        def step(c, _):
            q_c = q_buf[lanes(c), :]
            top = jnp.full((8, CW), NEG, F32)
            for e in range(ENT):
                raw = dot_nt(ksel[h, e * hb:(e + 1) * hb, :], q_c) * (FACTOR * LOG2E)
                if e == 0:
                    seen = key_row <= (col + c * CW) // groups
                else:
                    seen = key_row < vis_ref[0, e - 1]
                raw = jnp.where(seen, raw, NEG)
                s_buf[c, h, e] = raw
                top = jnp.maximum(top, jnp.max(eights(raw), axis=0))
            top = jnp.broadcast_to(jnp.max(top, axis=0, keepdims=True), (8, CW))
            total = jnp.zeros((8, CW), F32)
            for e in range(ENT):
                expo = jnp.exp2(s_buf[c, h, e] - top[:1])
                s_buf[c, h, e] = expo
                total = total + jnp.sum(eights(expo), axis=0)
            top_buf[c, h] = top
            sum_buf[c, h] = jnp.broadcast_to(jnp.sum(total, axis=0, keepdims=True), (8, CW))
            return 0

        lax.fori_loop(0, chunks, step, 0)

    near = range(part_of[hz])
    rest = range(part_of[hz], len(parts))
    for part in near:
        collect(0, part)
        collect(1, part)
    collected(0, near)
    select_pages(0, ksel, 0)
    loads[3].wait()
    loads[5].wait()
    scores(0)
    for part in rest:
        collect(0, part)
        collect(1, part)
    collected(1, near)
    select_pages(1, vsel, 0)
    transposed(vsel, vt_sel, 0)
    transposed(ksel, kt_sel, 0)
    collected(0, rest)
    select_pages(0, ksel, 1)
    scores(1)
    collected(1, rest)
    select_pages(1, vsel, 1)
    transposed(vsel, vt_sel, 1)

    def values(c, _):
        g_c = g_buf[lanes(c), :]
        top = jnp.maximum(top_buf[c, 0], top_buf[c, 1])
        scale = [jnp.exp2(top_buf[c, h] - top) for h in range(2)]
        inverse = 1.0 / (sum_buf[c, 0] * scale[0] + sum_buf[c, 1] * scale[1])
        out_t = jnp.zeros((HD, CW), F32)
        for h in range(2):
            factor = (scale[h] * inverse)[:1]
            for e in range(ENT):
                w = s_buf[c, h, e] * factor
                s_buf[c, h, e] = w
                ds_buf[c, h, e * hb:(e + 1) * hb, :] = w.astype(BF16)
            w_b = ds_buf[c, h]
            acc[1, h, :ENT] += dot(w_b, g_c).reshape(ENT, hb, HD)
            out_t = out_t + dot(vt_sel[h], w_b)
        out_b = out_t.astype(BF16)
        att_ref[lanes(c), :] = out_b.T
        delta = jnp.sum(out_b.astype(F32) * gt_buf[c].astype(F32), axis=0, keepdims=True)
        delta_buf[c] = jnp.broadcast_to(delta, (8, CW))
        return 0

    lax.fori_loop(0, chunks, values, 0)

    def slot_sum(t, h, page):
        return acc[t, h, slot_of[0, page]] + acc[t, h, slot_of[1, page]]

    def partner_send(t, h, a):
        return remote(dsend.at[t, h, a], prec.at[t, h, a], dd_send.at[0], dd_recv.at[t, h, a], partner, z)

    def first_send(t, h, a):
        to = spot(t, h, a, 0) * 2 + core
        return remote(rsend.at[t, h, a], rrec.at[t, h, a], r1_send.at[0], r1_recv.at[t, h], to, z)

    def second_send(t, h, b):
        to = spot(t, h, 0, b) * 2 + core
        return remote(ssend.at[t, h, b], srec.at[t, h, b], r2_send.at[0], r2_recv.at[t, h], to, z)

    def to_partner(t, h):
        for a in far_first(size_a(t, h)) + [0]:
            for b in range(size_b(t, h)):
                dsend[t, h, a, b] = slot_sum(t, h, spot(t, h, a, b) * 2 + (1 - core)).astype(BF16)
            partner_send(t, h, a).start()

    def mine(t, h, a, b):
        return slot_sum(t, h, spot(t, h, a, b) * 2 + core) + prec[t, h, a, b].astype(F32)

    def first_step(t, h, lo=0, hi=None):
        for a in far_first(size_a(t, h))[lo:hi]:
            partner_send(t, h, a).wait_recv()
            for b in range(size_b(t, h)):
                rsend[t, h, a, b] = mine(t, h, a, b).astype(BF16)
            first_send(t, h, a).start()

    def gathered(t, h, b):
        total = mine(t, h, 0, b)
        for a in range(1, size_a(t, h)):
            total = total + rrec[t, h, a, b].astype(F32)
        return total

    def second_step(t, h):
        partner_send(t, h, 0).wait_recv()
        here = rrec.at[t, h, pl.ds(1, size_a(t, h) - 1)]
        remote(here, here, r1_send.at[0], r1_recv.at[t, h], partner, z).wait_recv()
        for b in far_first(size_b(t, h)):
            ssend[t, h, b] = gathered(t, h, b).astype(BF16)
            second_send(t, h, b).start()

    def zb_copy(t, j):
        back = slot_at[(nz - rel[j]) % nz]
        return remote(fin.at[t, j], zrec.at[t, back], zb_send.at[0], zb_recv.at[t], seq, lax.rem(z + rel[j], nz))

    def finish(t, h):
        total = acc[t, h, 0] + gathered(t, h, 0)
        here = srec.at[t, h, pl.ds(1, size_b(t, h) - 1)]
        remote(here, here, r2_send.at[0], r2_recv.at[t, h], partner, z).wait_recv()
        for b in range(1, size_b(t, h)):
            total = total + srec[t, h, b].astype(F32)
        if t == 0:
            total = total * FACTOR
        fin[t, h * hz:(h + 1) * hz] = total.astype(BF16).reshape(hz, sub, HD)
        for j in range((h + 1) * hz - 1, h * hz - 1, -1):
            if j == 0:
                zrec[t, 0] = fin[t, 0]
            else:
                zb_copy(t, j).start()

    def result(t, out_ref):
        here = zrec.at[t, pl.ds(1, nz - 1)]
        remote(here, here, zb_send.at[0], zb_recv.at[t], seq, lax.rem(z + 1, nz)).wait_recv()
        out_ref[...] = dot(from_slots, zrec[t].reshape(BLK, HD)).astype(BF16)

    def grads(h):
        def step(c, _):
            g_c = g_buf[lanes(c), :]
            delta = delta_buf[c][:1]
            for e in range(ENT):
                part = pl.ds(e * hb, hb)
                ds_buf[c, h, part] = (s_buf[c, h, e] * (dot_nt(vsel[h, part], g_c) - delta)).astype(BF16)
            acc[0, h, :ENT] += dot(ds_buf[c, h], q_buf[lanes(c), :]).reshape(ENT, hb, HD)
            return 0

        lax.fori_loop(0, chunks, step, 0)

    def query_grads(c, _):
        dq_t = dot(kt_sel[0], ds_buf[c, 0]) + dot(kt_sel[1], ds_buf[c, 1])
        qg_ref[lanes(c), :] = (dq_t * FACTOR).T.astype(BF16)
        return 0

    to_partner(1, 1)
    to_partner(1, 0)
    grads(1)
    to_partner(0, 1)
    first_step(1, 1)
    first_step(1, 0)
    grads(0)
    to_partner(0, 0)
    first_step(0, 1)
    transposed(ksel, kt_sel, 1)
    first_step(0, 0)
    lax.fori_loop(0, chunks, query_grads, 0)
    second_step(1, 1)
    second_step(1, 0)
    second_step(0, 1)
    finish(1, 1)
    second_step(0, 0)
    finish(1, 0)
    finish(0, 1)
    finish(0, 0)
    result(1, vg_ref)
    result(0, kg_ref)


    def sent(ref, sem):
        remote(ref, ref, sem, r2_recv.at[0, 0], partner, z).wait_send()

    sent(zsrc.at[:, pl.ds(1, nz - 1)], z_send.at[0])
    sent(dsend, dd_send.at[0])
    sent(rsend.at[:, :, pl.ds(1, nx - 1)], r1_send.at[0])
    sent(ssend.at[:, :, pl.ds(1, nx - 1)], r2_send.at[0])
    sent(fin.at[:, pl.ds(1, nz - 1)], zb_send.at[0])
    for t in range(2):
        sent(pages[t][0].at[pl.ds(0, nx - 1), pl.ds(0, 2), 0], la_send.at[t])
        sent(pages[t][0].at[pl.ds(0, ny - 1)], pa_send.at[t])
        sent(pages[t][0], fw_send.at[t])


def emit(*refs):
    n = (len(refs) - 1) // 2
    copies = [pltpu.make_async_copy(refs[i], refs[n + i], refs[-1].at[i]) for i in range(n)]
    for copy in copies:
        copy.start()
    for copy in copies:
        copy.wait()


def per_device(nx, ny, nz, queries, key_store, value_store, upstream, fork_pages, fork_visible):
    groups = queries.shape[1]
    rows = BLK * groups
    chunks = rows // CW
    nc = nx * ny
    sub = BLK // nz
    hb = BLK // 2
    nm = max(nx, ny)
    dma = pltpu.SemaphoreType.DMA
    vmem = pl.BlockSpec(memory_space=pltpu.VMEM)
    hbm = pl.BlockSpec(memory_space=pltpu.HBM)
    big = jax.ShapeDtypeStruct((rows, HD), BF16)
    small = jax.ShapeDtypeStruct((BLK, HD), BF16)
    outs = (big, big, small, small)
    results = pl.pallas_call(
        functools.partial(kernel, nx, ny, nz, groups),
        out_shape=tuple(pltpu.VMEM(o.shape, BF16) for o in outs),
        in_specs=[hbm] * 6,
        out_specs=(vmem,) * 4,
        scratch_shapes=[
            pltpu.VMEM((2, BLK, HD), BF16),
            pltpu.VMEM((rows, HD), BF16),
            pltpu.VMEM((rows, HD), BF16),
            pltpu.VMEM((chunks, HD, CW), BF16),
            pltpu.VMEM((chunks, 8, CW), F32),
            pltpu.VMEM((chunks, 2, 8, CW), F32),
            pltpu.VMEM((chunks, 2, 8, CW), F32),
            pltpu.VMEM((2, nz, sub, HD), BF16),
            pltpu.VMEM((ny, nx, 2, nz // 2, sub, HD), BF16),
            pltpu.VMEM((ny, nx, 2, nz // 2, sub, HD), BF16),
            pltpu.VMEM((ny, nx, 2, nz // 2, sub, HD), BF16),
            pltpu.VMEM((ny, nx, 2, nz // 2, sub, HD), BF16),
            pltpu.VMEM((2, ENT * hb, HD), BF16),
            pltpu.VMEM((2, ENT * hb, HD), BF16),
            pltpu.VMEM((2, HD, ENT * hb), BF16),
            pltpu.VMEM((2, HD, ENT * hb), BF16),
            pltpu.VMEM((chunks, 2, ENT, hb, CW), F32),
            pltpu.VMEM((chunks, 2, ENT * hb, CW), BF16),
            pltpu.VMEM((2, 2, ENT + 1, hb, HD), F32),
            pltpu.SMEM((1, FORKS), jnp.int32),
            pltpu.SMEM((1, FORKS), jnp.int32),
            pltpu.SMEM((2, 2 * nc), jnp.int32),
            pltpu.VMEM((2, 2, nm, nm, hb, HD), BF16),
            pltpu.VMEM((2, 2, nm, nm, hb, HD), BF16),
            pltpu.VMEM((2, 2, nm, nm, hb, HD), BF16),
            pltpu.VMEM((2, 2, nm, nm, hb, HD), BF16),
            pltpu.VMEM((2, 2, nm, hb, HD), BF16),
            pltpu.VMEM((2, 2, nm, hb, HD), BF16),
            pltpu.VMEM((2, nz, sub, HD), BF16),
            pltpu.VMEM((2, nz, sub, HD), BF16),
            dma((6,)),
            dma((1,)), dma((2, 5)),
            dma((2,)), dma((2, 5)),
            dma((2,)), dma((2, 5)),
            dma((2,)), dma((2, 5)),
            dma((1,)), dma((2, 2, nm)),
            dma((1,)), dma((2, 2)),
            dma((1,)), dma((2, 2)),
            dma((1,)), dma((2,)),
        ],
        compiler_params=pltpu.CompilerParams(
            collective_id=0, has_side_effects=True
        ),
    )(
        fork_pages, fork_visible,
        key_store.reshape(BLK, HD), value_store.reshape(BLK, HD),
        queries.reshape(rows, HD), upstream.reshape(rows, HD),
    )
    att, qg, kg, vg = pl.pallas_call(
        emit,
        out_shape=outs,
        in_specs=[vmem] * 4,
        out_specs=(hbm,) * 4,
        scratch_shapes=[dma((4,))],
        compiler_params=pltpu.CompilerParams(vmem_limit_bytes=4 * 2**20),
    )(*results)
    return (
        att.reshape(queries.shape), qg.reshape(queries.shape),
        kg.reshape(key_store.shape), vg.reshape(value_store.shape),
    )


def solution(mesh):
    nc = mesh.shape["seq"] // 2
    nx = 1
    while nx * nx < nc:
        nx *= 2
    placed = (
        P("seq", "head", None),
        P(("seq", "head"), None, None),
        P(("seq", "head"), None, None),
        P("seq", "head", None),
        P("seq", None),
        P("seq", None),
    )
    return jax.shard_map(
        functools.partial(per_device, nx, nc // nx, mesh.shape["head"]),
        mesh=mesh,
        in_specs=placed,
        out_specs=(
            P("seq", "head", None),
            P("seq", "head", None),
            P(("seq", "head"), None, None),
            P(("seq", "head"), None, None),
        ),
        check_vma=False,
    )
```
